512 devices in a mesh: dp: 8 (over x, core), ctx: 64 (over y, z).
Axes of the slice: x: 4, y: 4, z: 16, core: 2. Of those that a mesh axis runs over, the one named last changes fastest.
Arguments:
- queries: bfloat16 [32, 65536, 128], P(None, ('dp', 'ctx')), parts along dimension 1, may hold values from -150 to 150
- query_pos: bfloat16 [32, 65536, 64], P(None, ('dp', 'ctx')), parts along dimension 1, may hold values from -300 to 300
- key_values: bfloat16 [4, 2, 65536, 128], P(None, None, ('dp', 'ctx')), parts along dimension 2, may hold values from -20 to 20
- latent: bfloat16 [65536, 512], P(('dp', 'ctx')), parts along dimension 0, may hold values from -6 to 6
- key_pos: bfloat16 [65536, 64], P(('dp', 'ctx')), parts along dimension 0, may hold values from -4 to 4
- key_upward_matrix: bfloat16 [32, 128, 512], P(None, None, 'ctx'), may hold values from -0.5 to 0.5
- value_upward_matrix: bfloat16 [32, 512, 128], P(None, 'ctx'), may hold values from -1 to 1
- segment_ids: int32 [65536], P(('dp', 'ctx')), parts along dimension 0, may hold values from 0 to 63, never falling along the last dimension, each value on 1 to 256 neighbouring positions
Outputs:
- student_out: bfloat16 [32, 65536, 128], P(None, ('dp', 'ctx')), parts along dimension 1
- token_error: float32 [65536], P(('dp', 'ctx')), parts along dimension 0
The draws below stay inside these ranges and needn't reach their ends.
There are 8 independent parts, one for each index of `dp`. The reference program is written for one: setup_inputs(seed, part) draws one part's arguments, and reference() takes and returns one part's arrays. A program takes and returns all parts, laid end to end along the dimension named above; an argument that names none is the same for every part. Nothing has to cross between parts.
Inputs may be any that keep to these rules, and one draw needn't show every extreme that they name: `segment_ids`: each document covers at most 256 consecutive positions; ids never fall along the sequence.
All inputs are finite; a program needn't handle non-finite values.
Results may differ from the reference program's by a relative error of at most 0.0071.
Values may be sent and summed in bfloat16 or wider, within the bound.
No kernel may reach another device: no remote copies, remote signals or barrier semaphores. Data moves between devices by JAX's collectives and lax.ppermute only.
A program may use at most 64 MiB of HBM per device.

```python
import math
import jax
import jax.numpy as jnp
import numpy as np
from jax import lax

HEADS = 32
KV_HEADS = 4
HEAD_DIM = 128
LATENT = 512
ROPE_DIM = 64
TOK_DEV = 128
REACH = 2
TOKENS = 8192
DOC_MOST = 256
DOCS = 64


def joint_draw(key):
    base = jax.random.fold_in(key, 11)
    streams = jax.random.split(base, 4)
    queries = jnp.clip(jax.random.normal(streams[0], (HEADS, TOKENS, HEAD_DIM), jnp.float32), -5.0, 5.0)
    pair = jnp.clip(jax.random.normal(streams[1], (KV_HEADS, 2, TOKENS, HEAD_DIM), jnp.float32), -5.0, 5.0)
    pair = pair * jnp.array([1.0, 4.0], jnp.float32).reshape(1, 2, 1, 1)
    query_pos = jnp.clip(jax.random.normal(streams[2], (HEADS, TOKENS, ROPE_DIM), jnp.float32), -4.0, 4.0)
    key_pos = jnp.clip(jax.random.normal(streams[3], (TOKENS, ROPE_DIM), jnp.float32), -4.0, 4.0)
    return (queries, pair, query_pos, key_pos)


def draw_queries(key, part):
    return joint_draw(key)[0].astype(jnp.bfloat16)


def draw_key_values(key, part):
    return joint_draw(key)[1].astype(jnp.bfloat16)


def draw_query_pos(key, part):
    return joint_draw(key)[2].astype(jnp.bfloat16)


def draw_key_pos(key, part):
    return joint_draw(key)[3].astype(jnp.bfloat16)


def levels(rng, extent, cuts, smallest, high):
    factor_of = 1.0
    for position, blocks in cuts:
        draws = jax.random.uniform(jax.random.fold_in(jax.random.fold_in(rng, 6), position), (blocks,), jnp.float32, smallest / len(cuts), high / len(cuts))
        factor_of = factor_of * jnp.repeat(jnp.exp(draws), extent[position] // blocks).reshape((-1,) + (1,) * (len(extent) - 1 - position))
    return factor_of


def length_profile(count, total, most, slope):
    portions = [(1 << 20) // math.isqrt(rank ** slope) + 1 for rank in range(2, count + 1)]
    surplus, holding = total - most - (count - 1), [1] * (count - 1)
    while surplus > 0:
        candidates = [i for i in range(count - 1) if holding[i] < most]
        pool, remaining = sum([portions[i] for i in candidates]), surplus
        for i in candidates:
            more = min(most - holding[i], max(1, remaining * portions[i] // pool), surplus)
            holding[i] = holding[i] + more
            surplus = surplus - more
    return np.array([most] + holding)


def uneven_parts(own_key, number_of, total, most, skew):
    if number_of == 2:
        one = jax.random.randint(own_key, (), max(1, total - most), min(most, total - 1) + 1)
        return jnp.stack([one, total - one])
    lengths = jnp.asarray(length_profile(number_of, total, most, skew), jnp.int32)
    couples = (number_of - 1) // 2
    source_of, sink = lengths[1:1 + 2 * couples:2], lengths[2:2 + 2 * couples:2]
    room = jnp.minimum(source_of - 1, most - sink)
    passed = jax.random.randint(jax.random.fold_in(own_key, 1), (couples,), 0, 1 << 20) % (room + 1)
    lengths = lengths.at[1:1 + 2 * couples:2].set(source_of - passed).at[2:2 + 2 * couples:2].set(sink + passed)
    return lengths[jax.random.permutation(jax.random.fold_in(own_key, 2), number_of)]


def normal_values(own_key, dims, deviation, most, cuts=(), kind=jnp.bfloat16):
    level = levels(own_key, dims, cuts, -0.22, 0.18) if cuts else 1.0
    entries = jax.random.normal(own_key, dims, jnp.float32) * deviation * level
    return jnp.minimum(jnp.maximum(entries, -most), most).astype(kind)


def setup_inputs(seed: int = 0, part: int = 0) -> dict:
    key_list = jax.random.split(jax.random.key(seed), 9)
    part_splits = jax.random.split(jax.random.fold_in(key_list[8], part), 9)
    return {
        "queries": draw_queries(jax.random.fold_in(jax.random.fold_in(key_list[8], part), 71), part),
        "query_pos": draw_query_pos(jax.random.fold_in(jax.random.fold_in(key_list[8], part), 71), part),
        "key_values": draw_key_values(jax.random.fold_in(jax.random.fold_in(key_list[8], part), 71), part),
        "latent": normal_values(part_splits[3], (TOKENS, LATENT), 1.0, 6.0, ((0, 64),)),
        "key_pos": draw_key_pos(jax.random.fold_in(jax.random.fold_in(key_list[8], part), 71), part),
        "key_upward_matrix": normal_values(key_list[5], (HEADS, HEAD_DIM, LATENT), HEAD_DIM ** -0.5, 0.5, ((2, 64),)),
        "value_upward_matrix": normal_values(key_list[6], (HEADS, LATENT, HEAD_DIM), (LATENT // 16) ** -0.5, 1.0, ((1, 64),)),
        "segment_ids": jnp.searchsorted(jnp.cumsum(uneven_parts(part_splits[7], DOCS, TOKENS, DOC_MOST, 2)), jnp.arange(TOKENS), side="right").astype(jnp.int32),
    }


def masked_softmax(scores, allowed):
    scores = jnp.where(allowed, scores, -jnp.inf)
    highest = lax.optimization_barrier(jnp.max(scores, axis=-1, keepdims=True))
    raised = jnp.exp(scores - highest)
    return raised / lax.optimization_barrier(jnp.sum(raised, axis=-1, keepdims=True))

def reference(queries, query_pos, key_values, latent, key_pos, key_upward_matrix, value_upward_matrix, segment_ids):
    reach_len = REACH * TOK_DEV
    window = reach_len + TOK_DEV
    groups = HEADS // KV_HEADS
    pair_padded = jnp.pad(key_values, ((0, 0), (0, 0), (reach_len, 0), (0, 0)))
    latent_padded = jnp.pad(latent, ((reach_len, 0), (0, 0)))
    pos_padded = jnp.pad(key_pos, ((reach_len, 0), (0, 0)))
    seg_padded = jnp.pad(segment_ids, (reach_len, 0))
    teacher_scale = 1.0 / math.sqrt(HEAD_DIM)
    student_scale = 1.0 / math.sqrt(HEAD_DIM + ROPE_DIM)
    keys_up = key_upward_matrix.astype(jnp.float32)
    values_up = value_upward_matrix.astype(jnp.float32)

    def one_block(block_id):
        first_row = (block_id * TOK_DEV).astype(jnp.int32)
        query_index = first_row + jnp.arange(TOK_DEV, dtype=jnp.int32)
        key_index = first_row - reach_len + jnp.arange(window, dtype=jnp.int32)
        query_seg = lax.dynamic_slice_in_dim(segment_ids, first_row, TOK_DEV, 0)
        key_seg = lax.dynamic_slice_in_dim(seg_padded, first_row, window, 0)
        allowed = (key_seg[None, :] == query_seg[:, None]) & (key_index[None, :] <= query_index[:, None]) & (key_index[None, :] >= 0)
        current_query_block = lax.dynamic_slice_in_dim(queries, first_row, TOK_DEV, 1).astype(jnp.float32)
        qpos_block = lax.dynamic_slice_in_dim(query_pos, first_row, TOK_DEV, 1).astype(jnp.float32)
        pair_block = lax.dynamic_slice_in_dim(pair_padded, first_row, window, 2).astype(jnp.float32)
        grouped = current_query_block.reshape(KV_HEADS, groups, TOK_DEV, HEAD_DIM)
        teacher_scores = jnp.einsum('kgtd,kld->kgtl', grouped, pair_block[:, 0]) * teacher_scale
        teacher_weights = masked_softmax(teacher_scores, allowed[None, None]).astype(jnp.bfloat16)
        teacher_out = jnp.einsum('kgtl,kld->kgtd', teacher_weights.astype(jnp.float32), pair_block[:, 1])
        teacher_out = teacher_out.astype(jnp.bfloat16).reshape(HEADS, TOK_DEV, HEAD_DIM)
        query_latent = jnp.einsum('htd,hdc->htc', current_query_block, keys_up).astype(jnp.bfloat16)
        latent_block = lax.dynamic_slice_in_dim(latent_padded, first_row, window, 0).astype(jnp.float32)
        kpos_block = lax.dynamic_slice_in_dim(pos_padded, first_row, window, 0).astype(jnp.float32)
        student_scores = jnp.einsum('htc,lc->htl', query_latent.astype(jnp.float32), latent_block)
        student_scores = (student_scores + jnp.einsum('htp,lp->htl', qpos_block, kpos_block)) * student_scale
        student_weights = masked_softmax(student_scores, allowed[None]).astype(jnp.bfloat16)
        latent_out = jnp.einsum('htl,lc->htc', student_weights.astype(jnp.float32), latent_block).astype(jnp.bfloat16)
        student_out = jnp.einsum('htc,hcd->htd', latent_out.astype(jnp.float32), values_up).astype(jnp.bfloat16)
        return (student_out, teacher_out)
    students, teachers = lax.map(one_block, jnp.arange(TOKENS // TOK_DEV, dtype=jnp.int32))
    student_out = jnp.transpose(students, (1, 0, 2, 3)).reshape(HEADS, TOKENS, HEAD_DIM)
    teacher_out = jnp.transpose(teachers, (1, 0, 2, 3)).reshape(HEADS, TOKENS, HEAD_DIM)
    difference = student_out.astype(jnp.float32) - teacher_out.astype(jnp.float32)
    token_error = lax.optimization_barrier(jnp.mean(difference * difference, axis=(0, 2)))
    return (student_out, token_error)
```

```python
import functools
import math

import jax
import jax.numpy as jnp
from jax import lax
from jax.experimental import pallas as pl
from jax.experimental.pallas import tpu as pltpu
from jax.sharding import Mesh
from jax.sharding import PartitionSpec as P

REACH = 2
GROUP = 4
BLOCK = 128
MASKED = -1e30
LOG2E = math.log2(math.e)


def to_all(a, axis):
    sizes = [lax.axis_size(k) for k in ((axis,) if isinstance(axis, str) else axis)]
    n = math.prod(sizes)
    got = lax.all_to_all(jnp.broadcast_to(a[None], (n, *a.shape)), axis, 0, 0, tiled=True)
    return got.reshape(*sizes, *a.shape)


def from_behind(block):
    axes = ("y", "z")
    n = math.prod(lax.axis_size(a) for a in axes)
    return lax.ppermute(block, axes, [(i - 1, i) for i in range(1, n)])


def partner(a):
    return lax.ppermute(a, "core", [(0, 1), (1, 0)])


def gather_z(part):
    line = to_all(part, "z")
    line = jnp.transpose(line, (1, 2, 0, 3, 4))
    return line.reshape(*part.shape[:2], -1, part.shape[3])


def after(a, *others):
    return lax.optimization_barrier((a, *others))[0]


def nt(a, b):
    return lax.dot_general(a, b, (((1,), (1,)), ((), ())), preferred_element_type=jnp.float32)


def nn(a, b):
    return jnp.dot(a, b, preferred_element_type=jnp.float32)


def weights_of(scores, bias, scale):
    rows, keys = scores.shape
    t = (scores * (scale * LOG2E)).reshape(GROUP, BLOCK, keys) + bias[None]
    t = t.reshape(rows, keys)
    e = jnp.exp2(t - jnp.max(t, axis=-1, keepdims=True))
    return (e * (1.0 / jnp.sum(e, axis=-1, keepdims=True))).astype(jnp.bfloat16)


def attend(rope, at_ref, q, qpos, *refs):
    (kv2, kv1, kv0, la2, la1, la0, kp2, kp1, kp0, w_ref), refs = refs[:10], refs[10:]
    latent_out, teacher_out, lat, bias, ql = refs
    width = la0.shape[0] * BLOCK
    window = (REACH + 1) * BLOCK

    @pl.when(pl.program_id(0) == 0)
    def _():
        segs = []
        for b, (la, kp) in enumerate(((la2, kp2), (la1, kp1), (la0, kp0))):
            rows = slice(b * BLOCK, (b + 1) * BLOCK)
            for c in range(la.shape[0]):
                lat[rows, c * BLOCK : (c + 1) * BLOCK] = la[c]
            both = kp[0]
            lane = lax.broadcasted_iota(jnp.int32, both.shape, 1)
            lat[rows, width:] = jnp.where(lane < rope, both, jnp.zeros_like(both))
            seg = both[:, rope : rope + 1].astype(jnp.float32)
            segs.append(jnp.broadcast_to(seg, (BLOCK, BLOCK)))
        key_seg = jnp.concatenate([s.T for s in segs], axis=1)
        query_seg = jnp.concatenate([segs[-1]] * (REACH + 1), axis=1)
        token = lax.broadcasted_iota(jnp.int32, (BLOCK, window), 0)
        key = lax.broadcasted_iota(jnp.int32, (BLOCK, window), 1) - REACH * BLOCK
        allowed = (key_seg == query_seg) & (key <= token) & (key + at_ref[1] >= 0)
        bias[...] = jnp.where(allowed, 0.0, MASKED)
        ql[:, width:] = jnp.zeros((ql.shape[0], BLOCK), jnp.bfloat16)

    for h in range(GROUP):
        w = weight_of(w_ref, h)
        ql[h * BLOCK : (h + 1) * BLOCK, :width] = nt(q[h], w).astype(jnp.bfloat16)
    ql[:, width : width + rope] = qpos[...].reshape(GROUP * BLOCK, rope)
    biases = bias[...]
    head_dim = q.shape[-1]
    p = weights_of(nt(ql[...], lat[...]), biases, 1.0 / math.sqrt(head_dim + rope))
    latent_out[0] = nn(p, lat[:, :width]).astype(jnp.bfloat16)

    keys = jnp.concatenate([kv2[0], kv1[0], kv0[0]], axis=0)
    values = jnp.concatenate([kv2[1], kv1[1], kv0[1]], axis=0)
    p = weights_of(nt(q[...].reshape(GROUP * BLOCK, head_dim), keys), biases, 1.0 / math.sqrt(head_dim))
    teacher_out[0] = nn(p, values).astype(jnp.bfloat16)


def weight_of(w, h):
    return w[0, :, h].reshape(w.shape[1] * BLOCK, w.shape[4])


def group_of(other):
    return lambda s, at: 2 * s + (1 - at[0] if other else at[0])


def weight_spec(w, start, count):
    return pl.BlockSpec((1, *w.shape[1:]), lambda s, i: (jnp.clip(s - start, 0, count - 1), 0, 0, 0, 0))


def run_attend(at_ref, queries, query_pos, bundles, w, rope, other):
    steps, chunks = w.shape[:2]
    head_dim = queries.shape[-1]
    rows = GROUP * BLOCK
    window = (REACH + 1) * BLOCK
    kv_rows = bundles[0].shape[0] - chunks - 1
    per_kv = queries.shape[0] // (kv_rows // 2) // GROUP
    group = group_of(other)
    kv = pl.BlockSpec((2, BLOCK, BLOCK), lambda s, i: (group(s, i) // per_kv, 0, 0))
    la = pl.BlockSpec((chunks, BLOCK, BLOCK), lambda s, i: (kv_rows // chunks, 0, 0))
    kp = pl.BlockSpec((1, BLOCK, BLOCK), lambda s, i: (kv_rows + chunks, 0, 0))
    flops = 2 * steps * rows * (head_dim * chunks * BLOCK + window * (2 * chunks * BLOCK + rope + 2 * head_dim))
    return pl.pallas_call(
        functools.partial(attend, rope),
        out_shape=(
            jax.ShapeDtypeStruct((steps, rows, chunks * BLOCK), jnp.bfloat16),
            jax.ShapeDtypeStruct((steps, rows, head_dim), jnp.bfloat16),
        ),
        grid_spec=pltpu.PrefetchScalarGridSpec(
            num_scalar_prefetch=1,
            grid=(steps,),
            in_specs=[
                pl.BlockSpec((GROUP, BLOCK, head_dim), lambda s, i: (group(s, i), 0, 0)),
                pl.BlockSpec((GROUP, BLOCK, rope), lambda s, i: (group(s, i), 0, 0)),
                kv, kv, kv, la, la, la, kp, kp, kp,
                weight_spec(w, 0, steps),
            ],
            out_specs=[
                pl.BlockSpec((1, rows, chunks * BLOCK), lambda s, i: (s, 0, 0)),
                pl.BlockSpec((1, rows, head_dim), lambda s, i: (s, 0, 0)),
            ],
            scratch_shapes=[
                pltpu.VMEM((window, (chunks + 1) * BLOCK), jnp.bfloat16),
                pltpu.VMEM((BLOCK, window), jnp.float32),
                pltpu.VMEM((rows, (chunks + 1) * BLOCK), jnp.bfloat16),
            ],
        ),
        cost_estimate=pl.CostEstimate(flops=flops * 4, bytes_accessed=steps * 3 * 2**20, transcendentals=0),
        name="attend",
    )(at_ref, queries, query_pos, *bundles, *bundles, *bundles, w)


def raise_up(count, heads, at_ref, low, teach, w_ref, *refs):
    acc_in = None if len(refs) == 2 else refs[1]
    out, acc = refs[-2:] if acc_in is None else refs[2:4]
    step = pl.program_id(0)

    @pl.when(step == 0)
    def _():
        acc[...] = jnp.zeros_like(acc) if acc_in is None else acc_in[...]

    total = acc[...]
    for h in range(GROUP):
        rows = slice(h * BLOCK, (h + 1) * BLOCK)
        o = nn(low[0, rows], weight_of(w_ref, h)).astype(jnp.bfloat16)
        out[h] = o
        d = o.astype(jnp.float32) - teach[0, rows].astype(jnp.float32)
        total = total + d * d
    acc[...] = total

    if acc_in is not None:

        @pl.when(step == count - 1)
        def _():
            error = refs[4]
            error[...] = jnp.sum(acc[...].T, axis=0, keepdims=True) * (1.0 / (heads * acc.shape[1]))


def run_raise(at_ref, low, teach, w, heads, other, earlier=()):
    count, rows, width = low.shape
    head_dim = teach.shape[-1]
    group = group_of(other)
    sums = pl.BlockSpec((BLOCK, head_dim), lambda s, i: (0, 0))
    out_shape = [
        jax.ShapeDtypeStruct((heads, BLOCK, head_dim), jnp.bfloat16),
        jax.ShapeDtypeStruct((BLOCK, head_dim), jnp.float32),
    ]
    out_specs = [pl.BlockSpec((GROUP, BLOCK, head_dim), lambda s, i: (group(s, i), 0, 0)), sums]
    in_specs = [
        pl.BlockSpec((1, rows, width), lambda s, i: (s, 0, 0)),
        pl.BlockSpec((1, rows, head_dim), lambda s, i: (s, 0, 0)),
        weight_spec(w, 0, count),
    ]
    aliases = {}
    if earlier:
        in_specs += [pl.BlockSpec(memory_space=pl.ANY), sums]
        out_shape.append(jax.ShapeDtypeStruct((1, BLOCK), jnp.float32))
        out_specs.append(pl.BlockSpec((1, BLOCK), lambda s, i: (0, 0)))
        aliases = {4: 0}
    return pl.pallas_call(
        functools.partial(raise_up, count, heads),
        out_shape=out_shape,
        grid_spec=pltpu.PrefetchScalarGridSpec(
            num_scalar_prefetch=1, grid=(count,), in_specs=in_specs, out_specs=out_specs
        ),
        input_output_aliases=aliases,
        cost_estimate=pl.CostEstimate(
            flops=8 * count * rows * width * head_dim, bytes_accessed=count * 2**20, transcendentals=0
        ),
        name="raise_up",
    )(at_ref, low, teach, w, *earlier)


def shards(queries, query_pos, key_values, latent, key_pos, key_up, value_up, segment_ids):
    heads, block, head_dim = queries.shape
    rope = key_pos.shape[1]
    x, core = lax.axis_index("x"), lax.axis_index("core")
    place = lax.axis_index("y") * lax.axis_size("z") + lax.axis_index("z")
    group = x * 2 + core

    k_part = lax.dynamic_slice_in_dim(key_up, group * GROUP, GROUP, 0).swapaxes(1, 2)
    v_part = lax.dynamic_slice_in_dim(value_up, group * GROUP, GROUP, 0)
    line = gather_z(jnp.stack([k_part, v_part]))

    tail = jnp.concatenate(
        [
            key_pos,
            segment_ids.astype(jnp.bfloat16)[:, None],
            jnp.zeros((block, BLOCK - rope - 1), jnp.bfloat16),
        ],
        axis=1,
    )
    bundle = jnp.concatenate(
        [
            key_values.reshape(-1, block, head_dim),
            jnp.moveaxis(latent.reshape(block, -1, BLOCK), 1, 0),
            tail[None],
        ],
        axis=0,
    )
    k_own = to_all(line[0], ("x", "y"))
    behind = from_behind(bundle)
    bundles = (from_behind(behind), behind, bundle)
    k_own = after(k_own, bundles[0])
    v_own = to_all(after(line[1], k_own), ("x", "y"))

    at = jnp.stack([core.astype(jnp.int32), (place * block).astype(jnp.int32)])
    k_other = partner(k_own)
    low, teach = run_attend(at, queries, query_pos, bundles, k_own, rope, 0)
    low_2, teach_2 = run_attend(at, queries, query_pos, bundles, after(k_other, low), rope, 1)
    v_own = after(v_own, low, low_2)
    v_other = partner(v_own)
    out, sums = run_raise(at, low, teach, v_own, heads, 0)
    out, _, error = run_raise(at, low_2, teach_2, after(v_other, sums), heads, 1, (out, sums))
    return out, error.reshape(block)


def solution(mesh):
    dp, ctx = mesh.devices.shape
    fine = Mesh(mesh.devices.reshape(dp // 2, 2, 4, ctx // 4), ("x", "core", "y", "z"))
    features = ("y", "z")
    tokens = ("x", "core", *features)
    placed = (
        P(None, tokens, None),
        P(None, tokens, None),
        P(None, None, tokens, None),
        P(tokens, None),
        P(tokens, None),
        P(None, None, features),
        P(None, features, None),
        P(tokens),
    )
    return jax.shard_map(
        shards,
        mesh=fine,
        in_specs=placed,
        out_specs=(P(None, tokens, None), P(tokens)),
        check_vma=False,
    )
```

```python
import functools
import math

import jax
import jax.numpy as jnp
from jax import lax
from jax.experimental import pallas as pl
from jax.experimental.pallas import tpu as pltpu
from jax.sharding import Mesh
from jax.sharding import PartitionSpec as P

REACH = 2
GROUP = 4
BLOCK = 128
MASKED = -1e30
LOG2E = math.log2(math.e)


def copies(a, n):
    return jnp.broadcast_to(a[None], (n, *a.shape))


def to_all(a, axis, spread=None):
    sizes = [lax.axis_size(k) for k in ((axis,) if isinstance(axis, str) else axis)]
    if spread is None:
        spread = copies(a, math.prod(sizes))
    got = lax.all_to_all(spread, axis, 0, 0, tiled=True)
    return got.reshape(*sizes, *a.shape)


def from_behind(block):
    axes = ("y", "z")
    n = math.prod(lax.axis_size(a) for a in axes)
    return lax.ppermute(block, axes, [(i - 1, i) for i in range(1, n)])


def partner(a):
    return lax.ppermute(a, "core", [(0, 1), (1, 0)])


def gather_z(part):
    line = to_all(part, "z")
    line = jnp.transpose(line, (1, 2, 0, 3, 4))
    return line.reshape(*part.shape[:2], -1, part.shape[3])


def after(a, *others):
    return lax.optimization_barrier((a, *others))[0]


def nt(a, b):
    return lax.dot_general(a, b, (((1,), (1,)), ((), ())), preferred_element_type=jnp.float32)


def nn(a, b):
    return jnp.dot(a, b, preferred_element_type=jnp.float32)


def weights_of(scores, bias, scale):
    rows, keys = scores.shape
    t = (scores * (scale * LOG2E)).reshape(GROUP, BLOCK, keys) + bias[None]
    t = t.reshape(rows, keys)
    e = jnp.exp2(t - jnp.max(t, axis=-1, keepdims=True))
    return (e * (1.0 / jnp.sum(e, axis=-1, keepdims=True))).astype(jnp.bfloat16)


def attend(rope, at_ref, q, qpos, *refs):
    (kv2, kv1, kv0, la2, la1, la0, kp2, kp1, kp0, w_ref), refs = refs[:10], refs[10:]
    latent_out, teacher_out, lat, bias, ql = refs
    width = la0.shape[0] * BLOCK
    window = (REACH + 1) * BLOCK

    @pl.when(pl.program_id(0) == 0)
    def _():
        segs = []
        for b, (la, kp) in enumerate(((la2, kp2), (la1, kp1), (la0, kp0))):
            rows = slice(b * BLOCK, (b + 1) * BLOCK)
            for c in range(la.shape[0]):
                lat[rows, c * BLOCK : (c + 1) * BLOCK] = la[c]
            both = kp[0]
            lane = lax.broadcasted_iota(jnp.int32, both.shape, 1)
            lat[rows, width:] = jnp.where(lane < rope, both, jnp.zeros_like(both))
            seg = both[:, rope : rope + 1].astype(jnp.float32)
            segs.append(jnp.broadcast_to(seg, (BLOCK, BLOCK)))
        key_seg = jnp.concatenate([s.T for s in segs], axis=1)
        query_seg = jnp.concatenate([segs[-1]] * (REACH + 1), axis=1)
        token = lax.broadcasted_iota(jnp.int32, (BLOCK, window), 0)
        key = lax.broadcasted_iota(jnp.int32, (BLOCK, window), 1) - REACH * BLOCK
        allowed = (key_seg == query_seg) & (key <= token) & (key + at_ref[1] >= 0)
        bias[...] = jnp.where(allowed, 0.0, MASKED)
        ql[:, width:] = jnp.zeros((ql.shape[0], BLOCK), jnp.bfloat16)

    for h in range(GROUP):
        w = weight_of(w_ref, h)
        ql[h * BLOCK : (h + 1) * BLOCK, :width] = nt(q[h], w).astype(jnp.bfloat16)
    ql[:, width : width + rope] = qpos[...].reshape(GROUP * BLOCK, rope)
    biases = bias[...]
    head_dim = q.shape[-1]
    p = weights_of(nt(ql[...], lat[...]), biases, 1.0 / math.sqrt(head_dim + rope))
    latent_out[0] = nn(p, lat[:, :width]).astype(jnp.bfloat16)

    keys = jnp.concatenate([kv2[0], kv1[0], kv0[0]], axis=0)
    values = jnp.concatenate([kv2[1], kv1[1], kv0[1]], axis=0)
    p = weights_of(nt(q[...].reshape(GROUP * BLOCK, head_dim), keys), biases, 1.0 / math.sqrt(head_dim))
    teacher_out[0] = nn(p, values).astype(jnp.bfloat16)


def weight_of(w, h):
    return w[0, :, h].reshape(w.shape[1] * BLOCK, w.shape[4])


def group_of(other):
    return lambda s, at: 2 * s + (1 - at[0] if other else at[0])


def weight_spec(w, start, count):
    return pl.BlockSpec((1, *w.shape[1:]), lambda s, i: (jnp.clip(s - start, 0, count - 1), 0, 0, 0, 0))


def run_attend(at_ref, queries, query_pos, bundles, w, rope, other):
    steps, chunks = w.shape[:2]
    head_dim = queries.shape[-1]
    rows = GROUP * BLOCK
    window = (REACH + 1) * BLOCK
    kv_rows = bundles[0].shape[0] - chunks - 1
    per_kv = queries.shape[0] // (kv_rows // 2) // GROUP
    group = group_of(other)
    kv = pl.BlockSpec((2, BLOCK, BLOCK), lambda s, i: (group(s, i) // per_kv, 0, 0))
    la = pl.BlockSpec((chunks, BLOCK, BLOCK), lambda s, i: (kv_rows // chunks, 0, 0))
    kp = pl.BlockSpec((1, BLOCK, BLOCK), lambda s, i: (kv_rows + chunks, 0, 0))
    flops = 2 * steps * rows * (head_dim * chunks * BLOCK + window * (2 * chunks * BLOCK + rope + 2 * head_dim))
    return pl.pallas_call(
        functools.partial(attend, rope),
        out_shape=(
            jax.ShapeDtypeStruct((steps, rows, chunks * BLOCK), jnp.bfloat16),
            jax.ShapeDtypeStruct((steps, rows, head_dim), jnp.bfloat16),
        ),
        grid_spec=pltpu.PrefetchScalarGridSpec(
            num_scalar_prefetch=1,
            grid=(steps,),
            in_specs=[
                pl.BlockSpec((GROUP, BLOCK, head_dim), lambda s, i: (group(s, i), 0, 0)),
                pl.BlockSpec((GROUP, BLOCK, rope), lambda s, i: (group(s, i), 0, 0)),
                kv, kv, kv, la, la, la, kp, kp, kp,
                weight_spec(w, 0, steps),
            ],
            out_specs=[
                pl.BlockSpec((1, rows, chunks * BLOCK), lambda s, i: (s, 0, 0)),
                pl.BlockSpec((1, rows, head_dim), lambda s, i: (s, 0, 0)),
            ],
            scratch_shapes=[
                pltpu.VMEM((window, (chunks + 1) * BLOCK), jnp.bfloat16),
                pltpu.VMEM((BLOCK, window), jnp.float32),
                pltpu.VMEM((rows, (chunks + 1) * BLOCK), jnp.bfloat16),
            ],
        ),
        cost_estimate=pl.CostEstimate(flops=flops * 4, bytes_accessed=steps * 3 * 2**20, transcendentals=0),
        name="attend",
    )(at_ref, queries, query_pos, *bundles, *bundles, *bundles, w)


def raise_up(count, heads, at_ref, low, teach, w_ref, *refs):
    acc_in = None if len(refs) == 2 else refs[1]
    out, acc = refs[-2:] if acc_in is None else refs[2:4]
    step = pl.program_id(0)

    @pl.when(step == 0)
    def _():
        acc[...] = jnp.zeros_like(acc) if acc_in is None else acc_in[...]

    total = acc[...]
    for h in range(GROUP):
        rows = slice(h * BLOCK, (h + 1) * BLOCK)
        o = nn(low[0, rows], weight_of(w_ref, h)).astype(jnp.bfloat16)
        out[h] = o
        d = o.astype(jnp.float32) - teach[0, rows].astype(jnp.float32)
        total = total + d * d
    acc[...] = total

    if acc_in is not None:

        @pl.when(step == count - 1)
        def _():
            error = refs[4]
            error[...] = jnp.sum(acc[...].T, axis=0, keepdims=True) * (1.0 / (heads * acc.shape[1]))


def run_raise(at_ref, low, teach, w, heads, other, earlier=()):
    count, rows, width = low.shape
    head_dim = teach.shape[-1]
    group = group_of(other)
    sums = pl.BlockSpec((BLOCK, head_dim), lambda s, i: (0, 0))
    out_shape = [
        jax.ShapeDtypeStruct((heads, BLOCK, head_dim), jnp.bfloat16),
        jax.ShapeDtypeStruct((BLOCK, head_dim), jnp.float32),
    ]
    out_specs = [pl.BlockSpec((GROUP, BLOCK, head_dim), lambda s, i: (group(s, i), 0, 0)), sums]
    in_specs = [
        pl.BlockSpec((1, rows, width), lambda s, i: (s, 0, 0)),
        pl.BlockSpec((1, rows, head_dim), lambda s, i: (s, 0, 0)),
        weight_spec(w, 0, count),
    ]
    aliases = {}
    if earlier:
        in_specs += [pl.BlockSpec(memory_space=pl.ANY), sums]
        out_shape.append(jax.ShapeDtypeStruct((1, BLOCK), jnp.float32))
        out_specs.append(pl.BlockSpec((1, BLOCK), lambda s, i: (0, 0)))
        aliases = {4: 0}
    return pl.pallas_call(
        functools.partial(raise_up, count, heads),
        out_shape=out_shape,
        grid_spec=pltpu.PrefetchScalarGridSpec(
            num_scalar_prefetch=1, grid=(count,), in_specs=in_specs, out_specs=out_specs
        ),
        input_output_aliases=aliases,
        cost_estimate=pl.CostEstimate(
            flops=8 * count * rows * width * head_dim, bytes_accessed=count * 2**20, transcendentals=0
        ),
        name="raise_up",
    )(at_ref, low, teach, w, *earlier)


def shards(queries, query_pos, key_values, latent, key_pos, key_up, value_up, segment_ids):
    heads, block, head_dim = queries.shape
    rope = key_pos.shape[1]
    x, core = lax.axis_index("x"), lax.axis_index("core")
    place = lax.axis_index("y") * lax.axis_size("z") + lax.axis_index("z")
    group = x * 2 + core

    k_part = lax.dynamic_slice_in_dim(key_up, group * GROUP, GROUP, 0).swapaxes(1, 2)
    v_part = lax.dynamic_slice_in_dim(value_up, group * GROUP, GROUP, 0)
    line = gather_z(jnp.stack([k_part, v_part]))

    tail = jnp.concatenate(
        [
            key_pos,
            segment_ids.astype(jnp.bfloat16)[:, None],
            jnp.zeros((block, BLOCK - rope - 1), jnp.bfloat16),
        ],
        axis=1,
    )
    bundle = jnp.concatenate(
        [
            key_values.reshape(-1, block, head_dim),
            jnp.stack(jnp.split(latent, latent.shape[1] // BLOCK, axis=1)),
            tail[None],
        ],
        axis=0,
    )
    behind = from_behind(bundle)
    bundles = (from_behind(behind), behind, bundle)
    plane = lax.axis_size("x") * lax.axis_size("y")
    k_own = to_all(line[0], ("x", "y"), after(copies(line[0], plane), bundles[0]))
    v_copies = copies(line[1], plane)
    k_own = after(k_own, v_copies)
    v_own = to_all(line[1], ("x", "y"), after(v_copies, k_own))

    at = jnp.stack([core.astype(jnp.int32), (place * block).astype(jnp.int32)])
    k_other = partner(k_own)
    low, teach = run_attend(at, queries, query_pos, bundles, k_own, rope, 0)
    low_2, teach_2 = run_attend(at, queries, query_pos, bundles, after(k_other, low), rope, 1)
    v_own = after(v_own, low, low_2)
    v_other = partner(v_own)
    out, sums = run_raise(at, low, teach, v_own, heads, 0)
    out, _, error = run_raise(at, low_2, teach_2, after(v_other, sums), heads, 1, (out, sums))
    return out, error.reshape(block)


def solution(mesh):
    dp, ctx = mesh.devices.shape
    fine = Mesh(mesh.devices.reshape(dp // 2, 2, 4, ctx // 4), ("x", "core", "y", "z"))
    features = ("y", "z")
    tokens = ("x", "core", *features)
    placed = (
        P(None, tokens, None),
        P(None, tokens, None),
        P(None, None, tokens, None),
        P(tokens, None),
        P(tokens, None),
        P(None, None, features),
        P(None, features, None),
        P(tokens),
    )
    return jax.shard_map(
        shards,
        mesh=fine,
        in_specs=placed,
        out_specs=(P(None, tokens, None), P(tokens)),
        check_vma=False,
    )
```

```python
import functools
import math

import jax
import jax.numpy as jnp
from jax import lax
from jax.experimental import pallas as pl
from jax.experimental.pallas import tpu as pltpu
from jax.sharding import Mesh
from jax.sharding import PartitionSpec as P

REACH = 2
GROUP = 4
BLOCK = 128
MASKED = -1e30
CHAIN = 4
TAIL_SEG = 64
LOG2E = math.log2(math.e)


def to_all(a, axis):
    sizes = [lax.axis_size(k) for k in ((axis,) if isinstance(axis, str) else axis)]
    n = math.prod(sizes)
    got = lax.all_to_all(jnp.broadcast_to(a[None], (n, *a.shape)), axis, 0, 0, tiled=True)
    return got.reshape(*sizes, *a.shape)


def from_behind(block):
    axes = ("y", "z")
    n = math.prod(lax.axis_size(a) for a in axes)
    return lax.ppermute(block, axes, [(i - 1, i) for i in range(1, n)])


def partner(a):
    return lax.ppermute(a, "core", [(0, 1), (1, 0)])


def gather_z(part):
    line = to_all(part, "z")
    line = jnp.transpose(line, (1, 2, 0, 3, 4))
    return line.reshape(*part.shape[:2], -1, part.shape[3])


def after(a, *others):
    return lax.optimization_barrier((a, *others))[0]


def nt(a, b):
    return lax.dot_general(a, b, (((1,), (1,)), ((), ())), preferred_element_type=jnp.float32)


def nn(a, b):
    return jnp.dot(a, b, preferred_element_type=jnp.float32)


def weights_of(scores, bias, scale):
    rows, keys = scores.shape
    t = (scores * (scale * LOG2E)).reshape(-1, BLOCK, keys) + bias[None]
    t = t.reshape(rows, keys)
    e = jnp.exp2(t - jnp.max(t, axis=-1, keepdims=True))
    return (e * (1.0 / jnp.sum(e, axis=-1, keepdims=True))).astype(jnp.bfloat16)


def teacher(at_ref, q, kv2, kv1, kv0, kp2, kp1, kp0, out, bias_out, bias):
    rope = TAIL_SEG

    @pl.when(pl.program_id(0) == 0)
    def _():
        segs = [
            jnp.broadcast_to(kp[0][:, rope : rope + 1].astype(jnp.float32), (BLOCK, BLOCK))
            for kp in (kp2, kp1, kp0)
        ]
        window = len(segs) * BLOCK
        key_seg = jnp.concatenate([s.T for s in segs], axis=1)
        query_seg = jnp.concatenate([segs[-1]] * len(segs), axis=1)
        token = lax.broadcasted_iota(jnp.int32, (BLOCK, window), 0)
        key = lax.broadcasted_iota(jnp.int32, (BLOCK, window), 1) - REACH * BLOCK
        allowed = (key_seg == query_seg) & (key <= token) & (key + at_ref[1] >= 0)
        bias[...] = jnp.where(allowed, 0.0, MASKED)
        bias_out[...] = bias[...]

    head_dim = q.shape[-1]
    keys = jnp.concatenate([kv2[0], kv1[0], kv0[0]], axis=0)
    values = jnp.concatenate([kv2[1], kv1[1], kv0[1]], axis=0)
    for rows in range(0, GROUP, CHAIN):
        p = weights_of(nt(q[rows : rows + CHAIN].reshape(CHAIN * BLOCK, head_dim), keys), bias[...], head_dim**-0.5)
        out[rows : rows + CHAIN] = nn(p, values).astype(jnp.bfloat16).reshape(CHAIN, BLOCK, head_dim)


def run_teacher(at_ref, queries, bundles, chunks):
    heads, block, head_dim = queries.shape
    kv_rows = bundles[0].shape[0] - chunks - 1
    per_kv = heads // (kv_rows // 2) // GROUP
    window = (REACH + 1) * BLOCK
    kv = pl.BlockSpec((2, BLOCK, BLOCK), lambda s, i: (s // per_kv, 0, 0))
    kp = pl.BlockSpec((1, BLOCK, BLOCK), lambda s, i: (kv_rows + chunks, 0, 0))
    group = pl.BlockSpec((GROUP, BLOCK, head_dim), lambda s, i: (s, 0, 0))
    return pl.pallas_call(
        teacher,
        out_shape=(
            jax.ShapeDtypeStruct(queries.shape, jnp.bfloat16),
            jax.ShapeDtypeStruct((BLOCK, window), jnp.float32),
        ),
        grid_spec=pltpu.PrefetchScalarGridSpec(
            num_scalar_prefetch=1,
            grid=(heads // GROUP,),
            in_specs=[group, kv, kv, kv, kp, kp, kp],
            out_specs=[group, pl.BlockSpec((BLOCK, window), lambda s, i: (0, 0))],
            scratch_shapes=[pltpu.VMEM((BLOCK, window), jnp.float32)],
        ),
        cost_estimate=pl.CostEstimate(
            flops=4 * heads * block * window * head_dim, bytes_accessed=4 * 2**20, transcendentals=0
        ),
        name="teacher",
    )(at_ref, queries, *bundles, *bundles)


def student(heads, rope, at_ref, q, qpos, la2, la1, la0, kp2, kp1, kp0, bias, teach, w, *refs):
    acc_in = refs[1] if len(refs) == 7 else None
    out, acc = refs[2:4] if acc_in is not None else refs[:2]
    lat, ql = refs[-2:]
    step = pl.program_id(0)
    width = la0.shape[0] * BLOCK
    head_dim = q.shape[-1]

    @pl.when(step == 0)
    def _():
        acc[...] = jnp.zeros_like(acc) if acc_in is None else acc_in[...]
        for b, (la, kp) in enumerate(((la2, kp2), (la1, kp1), (la0, kp0))):
            rows = slice(b * BLOCK, (b + 1) * BLOCK)
            for c in range(la.shape[0]):
                lat[rows, c * BLOCK : (c + 1) * BLOCK] = la[c]
            both = kp[0]
            lane = lax.broadcasted_iota(jnp.int32, both.shape, 1)
            lat[rows, width:] = jnp.where(lane < rope, both, jnp.zeros_like(both))
        ql[:, width:] = jnp.zeros((ql.shape[0], BLOCK), jnp.bfloat16)

    for h in range(GROUP):
        ql[h * BLOCK : (h + 1) * BLOCK, width : width + rope] = qpos[h].T
    total = acc[...]
    for first in range(0, GROUP, CHAIN):
        for h in range(first, first + CHAIN):
            w_k = w[0, :, 0, h].reshape(width, head_dim)
            ql[h * BLOCK : (h + 1) * BLOCK, :width] = nt(q[h], w_k).astype(jnp.bfloat16)
        scores = nt(ql[first * BLOCK : (first + CHAIN) * BLOCK], lat[...])
        p = weights_of(scores, bias[...], 1.0 / math.sqrt(head_dim + rope))
        low = nn(p, lat[:, :width]).astype(jnp.bfloat16)
        for h in range(first, first + CHAIN):
            w_v = w[0, :, 1, h].reshape(width, head_dim)
            o = nn(low[(h - first) * BLOCK : (h - first + 1) * BLOCK], w_v).astype(jnp.bfloat16)
            out[h] = o
            d = o.astype(jnp.float32) - teach[h].astype(jnp.float32)
            total = total + d * d
    acc[...] = total

    if acc_in is not None:

        @pl.when(step == pl.num_programs(0) - 1)
        def _():
            refs[4][...] = jnp.sum(acc[...].T, axis=0, keepdims=True) * (1.0 / (heads * head_dim))


def run_student(at_ref, queries, query_pos, bundles, bias, teach, w, other, earlier=()):
    heads, block, head_dim = queries.shape
    rope = query_pos.shape[1]
    steps, chunks = w.shape[:2]
    rows, window = GROUP * BLOCK, (REACH + 1) * BLOCK
    kv_rows = bundles[0].shape[0] - chunks - 1

    def group(s, at):
        return (2 * s + (1 - at[0] if other else at[0]), 0, 0)

    la = pl.BlockSpec((chunks, BLOCK, BLOCK), lambda s, i: (kv_rows // chunks, 0, 0))
    kp = pl.BlockSpec((1, BLOCK, BLOCK), lambda s, i: (kv_rows + chunks, 0, 0))
    heads_spec = pl.BlockSpec((GROUP, BLOCK, head_dim), group)
    sums = pl.BlockSpec((BLOCK, head_dim), lambda s, i: (0, 0))
    in_specs = [
        heads_spec,
        pl.BlockSpec((GROUP, rope, BLOCK), group),
        la, la, la, kp, kp, kp,
        pl.BlockSpec((BLOCK, window), lambda s, i: (0, 0)),
        heads_spec,
        pl.BlockSpec((1, *w.shape[1:]), lambda s, i: (s, 0, 0, 0, 0, 0)),
    ]
    out_shape = [
        jax.ShapeDtypeStruct(queries.shape, jnp.bfloat16),
        jax.ShapeDtypeStruct((BLOCK, head_dim), jnp.float32),
    ]
    out_specs = [heads_spec, sums]
    aliases = {}
    if earlier:
        in_specs += [pl.BlockSpec(memory_space=pl.ANY), sums]
        out_shape.append(jax.ShapeDtypeStruct((1, BLOCK), jnp.float32))
        out_specs.append(pl.BlockSpec((1, BLOCK), lambda s, i: (0, 0)))
        aliases = {12: 0}
    flops = 2 * steps * rows * (2 * head_dim * chunks * BLOCK + window * (2 * chunks * BLOCK + rope))
    return pl.pallas_call(
        functools.partial(student, heads, rope),
        out_shape=out_shape,
        grid_spec=pltpu.PrefetchScalarGridSpec(
            num_scalar_prefetch=1,
            grid=(steps,),
            in_specs=in_specs,
            out_specs=out_specs,
            scratch_shapes=[
                pltpu.VMEM((window, (chunks + 1) * BLOCK), jnp.bfloat16),
                pltpu.VMEM((rows, (chunks + 1) * BLOCK), jnp.bfloat16),
            ],
        ),
        input_output_aliases=aliases,
        cost_estimate=pl.CostEstimate(flops=4 * flops, bytes_accessed=8 * 2**20, transcendentals=0),
        name="student",
    )(at_ref, queries, query_pos, *bundles, *bundles, bias, teach, w, *earlier)


def shards(queries, query_pos, key_values, latent, key_pos, key_up, value_up, segment_ids):
    heads, block, head_dim = queries.shape
    rope = key_pos.shape[1]
    x, core = lax.axis_index("x"), lax.axis_index("core")
    place = lax.axis_index("y") * lax.axis_size("z") + lax.axis_index("z")
    group = x * 2 + core

    k_part = lax.dynamic_slice_in_dim(key_up, group * GROUP, GROUP, 0).swapaxes(1, 2)
    v_part = lax.dynamic_slice_in_dim(value_up, group * GROUP, GROUP, 0)
    line = gather_z(jnp.stack([k_part, v_part]))

    tail = jnp.concatenate(
        [
            key_pos,
            segment_ids.astype(jnp.bfloat16)[:, None],
            jnp.zeros((block, BLOCK - rope - 1), jnp.bfloat16),
        ],
        axis=1,
    )
    bundle = jnp.concatenate(
        [
            key_values.reshape(-1, block, head_dim),
            jnp.stack(jnp.split(latent, latent.shape[1] // BLOCK, axis=1)),
            tail[None],
        ],
        axis=0,
    )
    behind = from_behind(bundle)
    bundles = (from_behind(behind), behind, bundle)
    at = jnp.stack([core.astype(jnp.int32), (place * block).astype(jnp.int32)])
    own = to_all(line, ("x", "y"))
    teach, bias = run_teacher(at, queries, bundles, latent.shape[1] // BLOCK)
    own = after(own, teach)
    other = partner(own)
    with_keys = (at, queries, query_pos.swapaxes(1, 2), bundles, bias, teach)
    earlier = run_student(*with_keys, own, 0)
    out, _, error = run_student(*with_keys, after(other, earlier[1]), 1, earlier)
    return out, error.reshape(block)


def solution(mesh):
    dp, ctx = mesh.devices.shape
    fine = Mesh(mesh.devices.reshape(dp // 2, 2, 4, ctx // 4), ("x", "core", "y", "z"))
    features = ("y", "z")
    tokens = ("x", "core", *features)
    placed = (
        P(None, tokens, None),
        P(None, tokens, None),
        P(None, None, tokens, None),
        P(tokens, None),
        P(tokens, None),
        P(None, None, features),
        P(None, features, None),
        P(tokens),
    )
    return jax.shard_map(
        shards,
        mesh=fine,
        in_specs=placed,
        out_specs=(P(None, tokens, None), P(tokens)),
        check_vma=False,
    )
```

```python
import functools
import math

import jax
import jax.numpy as jnp
from jax import lax
from jax.experimental import pallas as pl
from jax.experimental.pallas import tpu as pltpu
from jax.sharding import Mesh
from jax.sharding import PartitionSpec as P

REACH = 2
GROUP = 4
BLOCK = 128
MASKED = -1e30
CHAIN = 4
TAIL_SEG = 64
LOG2E = math.log2(math.e)


def to_all(a, axis):
    sizes = [lax.axis_size(k) for k in ((axis,) if isinstance(axis, str) else axis)]
    n = math.prod(sizes)
    got = lax.all_to_all(jnp.broadcast_to(a[None], (n, *a.shape)), axis, 0, 0, tiled=True)
    return got.reshape(*sizes, *a.shape)


def across_y(block, z_from):
    ny, nz = lax.axis_size("y"), lax.axis_size("z")
    route = [((y - 1) * nz + z, y * nz + z) for y in range(1, ny) for z in range(z_from, nz)]
    return lax.ppermute(block, ("y", "z"), route)


def two_behind(block, crossed):
    nz = lax.axis_size("z")
    z = lax.axis_index("z")
    last = jnp.where(z == nz - 1, crossed, block)
    one = lax.ppermute(last, "z", [(i, (i + 1) % nz) for i in range(nz)])
    two = lax.ppermute(one, "z", [(i, i + 1) for i in range(nz - 1)])
    wrapped = lax.ppermute(crossed, "z", [(nz - 2, 0)])
    return last, one, jnp.where(z == 0, wrapped, two)


def partner(a):
    return lax.ppermute(a, "core", [(0, 1), (1, 0)])


def gather_z(part):
    line = to_all(part, "z")
    line = jnp.transpose(line, (1, 2, 0, 3, 4))
    return line.reshape(*part.shape[:2], -1, part.shape[3])


def after(a, *others):
    return lax.optimization_barrier((a, *others))[0]


def nt(a, b):
    return lax.dot_general(a, b, (((1,), (1,)), ((), ())), preferred_element_type=jnp.float32)


def nn(a, b):
    return jnp.dot(a, b, preferred_element_type=jnp.float32)


def weights_of(scores, bias, scale):
    rows, keys = scores.shape
    t = (scores * (scale * LOG2E)).reshape(-1, BLOCK, keys) + bias[None]
    t = t.reshape(rows, keys)
    e = jnp.exp2(t - jnp.max(t, axis=-1, keepdims=True))
    return (e * (1.0 / jnp.sum(e, axis=-1, keepdims=True))).astype(jnp.bfloat16)


def teacher(at_ref, q, kv2, kv1, kv0, kp2, kp1, kp0, out, bias_out, bias):
    rope = TAIL_SEG

    @pl.when(pl.program_id(0) == 0)
    def _():
        segs = [
            jnp.broadcast_to(kp[0][:, rope : rope + 1].astype(jnp.float32), (BLOCK, BLOCK))
            for kp in (kp2, kp1, kp0)
        ]
        window = len(segs) * BLOCK
        key_seg = jnp.concatenate([s.T for s in segs], axis=1)
        query_seg = jnp.concatenate([segs[-1]] * len(segs), axis=1)
        token = lax.broadcasted_iota(jnp.int32, (BLOCK, window), 0)
        key = lax.broadcasted_iota(jnp.int32, (BLOCK, window), 1) - REACH * BLOCK
        allowed = (key_seg == query_seg) & (key <= token) & (key + at_ref[1] >= 0)
        bias[...] = jnp.where(allowed, 0.0, MASKED)
        bias_out[...] = bias[...]

    head_dim = q.shape[-1]
    keys = jnp.concatenate([kv2[0], kv1[0], kv0[0]], axis=0)
    values = jnp.concatenate([kv2[1], kv1[1], kv0[1]], axis=0)
    for rows in range(0, GROUP, CHAIN):
        p = weights_of(nt(q[rows : rows + CHAIN].reshape(CHAIN * BLOCK, head_dim), keys), bias[...], head_dim**-0.5)
        out[rows : rows + CHAIN] = nn(p, values).astype(jnp.bfloat16).reshape(CHAIN, BLOCK, head_dim)


def run_teacher(at_ref, queries, bundles, chunks):
    heads, block, head_dim = queries.shape
    kv_rows = bundles[0].shape[0] - chunks - 1
    per_kv = heads // (kv_rows // 2) // GROUP
    window = (REACH + 1) * BLOCK
    kv = pl.BlockSpec((2, BLOCK, BLOCK), lambda s, i: (s // per_kv, 0, 0))
    kp = pl.BlockSpec((1, BLOCK, BLOCK), lambda s, i: (kv_rows + chunks, 0, 0))
    group = pl.BlockSpec((GROUP, BLOCK, head_dim), lambda s, i: (s, 0, 0))
    return pl.pallas_call(
        teacher,
        out_shape=(
            jax.ShapeDtypeStruct(queries.shape, jnp.bfloat16),
            jax.ShapeDtypeStruct((BLOCK, window), jnp.float32),
        ),
        grid_spec=pltpu.PrefetchScalarGridSpec(
            num_scalar_prefetch=1,
            grid=(heads // GROUP,),
            in_specs=[group, kv, kv, kv, kp, kp, kp],
            out_specs=[group, pl.BlockSpec((BLOCK, window), lambda s, i: (0, 0))],
            scratch_shapes=[pltpu.VMEM((BLOCK, window), jnp.float32)],
        ),
        cost_estimate=pl.CostEstimate(
            flops=4 * heads * block * window * head_dim, bytes_accessed=4 * 2**20, transcendentals=0
        ),
        name="teacher",
    )(at_ref, queries, *bundles, *bundles)


def student(heads, rope, at_ref, q, qpos, la2, la1, la0, kp2, kp1, kp0, bias, teach, w, *refs):
    acc_in = refs[1] if len(refs) == 7 else None
    out, acc = refs[2:4] if acc_in is not None else refs[:2]
    lat, ql = refs[-2:]
    step = pl.program_id(0)
    width = la0.shape[0] * BLOCK
    head_dim = q.shape[-1]

    @pl.when(step == 0)
    def _():
        acc[...] = jnp.zeros_like(acc) if acc_in is None else acc_in[...]
        for b, (la, kp) in enumerate(((la2, kp2), (la1, kp1), (la0, kp0))):
            rows = slice(b * BLOCK, (b + 1) * BLOCK)
            for c in range(la.shape[0]):
                lat[rows, c * BLOCK : (c + 1) * BLOCK] = la[c]
            both = kp[0]
            lane = lax.broadcasted_iota(jnp.int32, both.shape, 1)
            lat[rows, width:] = jnp.where(lane < rope, both, jnp.zeros_like(both))
        ql[:, width:] = jnp.zeros((ql.shape[0], BLOCK), jnp.bfloat16)

    for h in range(GROUP):
        ql[h * BLOCK : (h + 1) * BLOCK, width : width + rope] = qpos[h].T
    total = acc[...]
    for first in range(0, GROUP, CHAIN):
        for h in range(first, first + CHAIN):
            w_k = w[0, :, 0, h].reshape(width, head_dim)
            ql[h * BLOCK : (h + 1) * BLOCK, :width] = nt(q[h], w_k).astype(jnp.bfloat16)
        scores = nt(ql[first * BLOCK : (first + CHAIN) * BLOCK], lat[...])
        p = weights_of(scores, bias[...], 1.0 / math.sqrt(head_dim + rope))
        low = nn(p, lat[:, :width]).astype(jnp.bfloat16)
        for h in range(first, first + CHAIN):
            w_v = w[0, :, 1, h].reshape(width, head_dim)
            o = nn(low[(h - first) * BLOCK : (h - first + 1) * BLOCK], w_v).astype(jnp.bfloat16)
            out[h] = o
            d = o.astype(jnp.float32) - teach[h].astype(jnp.float32)
            total = total + d * d
    acc[...] = total

    if acc_in is not None:

        @pl.when(step == pl.num_programs(0) - 1)
        def _():
            refs[4][...] = jnp.sum(acc[...].T, axis=0, keepdims=True) * (1.0 / (heads * head_dim))


def run_student(at_ref, queries, query_pos, bundles, bias, teach, w, other, earlier=()):
    heads, block, head_dim = queries.shape
    rope = query_pos.shape[1]
    steps, chunks = w.shape[:2]
    rows, window = GROUP * BLOCK, (REACH + 1) * BLOCK
    kv_rows = bundles[0].shape[0] - chunks - 1

    def group(s, at):
        return (2 * s + (1 - at[0] if other else at[0]), 0, 0)

    la = pl.BlockSpec((chunks, BLOCK, BLOCK), lambda s, i: (kv_rows // chunks, 0, 0))
    kp = pl.BlockSpec((1, BLOCK, BLOCK), lambda s, i: (kv_rows + chunks, 0, 0))
    heads_spec = pl.BlockSpec((GROUP, BLOCK, head_dim), group)
    sums = pl.BlockSpec((BLOCK, head_dim), lambda s, i: (0, 0))
    in_specs = [
        heads_spec,
        pl.BlockSpec((GROUP, rope, BLOCK), group),
        la, la, la, kp, kp, kp,
        pl.BlockSpec((BLOCK, window), lambda s, i: (0, 0)),
        heads_spec,
        pl.BlockSpec((1, *w.shape[1:]), lambda s, i: (s, 0, 0, 0, 0, 0)),
    ]
    out_shape = [
        jax.ShapeDtypeStruct(queries.shape, jnp.bfloat16),
        jax.ShapeDtypeStruct((BLOCK, head_dim), jnp.float32),
    ]
    out_specs = [heads_spec, sums]
    aliases = {}
    if earlier:
        in_specs += [pl.BlockSpec(memory_space=pl.ANY), sums]
        out_shape.append(jax.ShapeDtypeStruct((1, BLOCK), jnp.float32))
        out_specs.append(pl.BlockSpec((1, BLOCK), lambda s, i: (0, 0)))
        aliases = {12: 0}
    flops = 2 * steps * rows * (2 * head_dim * chunks * BLOCK + window * (2 * chunks * BLOCK + rope))
    return pl.pallas_call(
        functools.partial(student, heads, rope),
        out_shape=out_shape,
        grid_spec=pltpu.PrefetchScalarGridSpec(
            num_scalar_prefetch=1,
            grid=(steps,),
            in_specs=in_specs,
            out_specs=out_specs,
            scratch_shapes=[
                pltpu.VMEM((window, (chunks + 1) * BLOCK), jnp.bfloat16),
                pltpu.VMEM((rows, (chunks + 1) * BLOCK), jnp.bfloat16),
            ],
        ),
        input_output_aliases=aliases,
        cost_estimate=pl.CostEstimate(flops=4 * flops, bytes_accessed=8 * 2**20, transcendentals=0),
        name="student",
    )(at_ref, queries, query_pos, *bundles, *bundles, bias, teach, w, *earlier)


def shards(queries, query_pos, key_values, latent, key_pos, key_up, value_up, segment_ids):
    heads, block, head_dim = queries.shape
    rope = key_pos.shape[1]
    x, core = lax.axis_index("x"), lax.axis_index("core")
    place = lax.axis_index("y") * lax.axis_size("z") + lax.axis_index("z")
    group = x * 2 + core

    tail = jnp.concatenate(
        [
            key_pos,
            segment_ids.astype(jnp.bfloat16)[:, None],
            jnp.zeros((block, BLOCK - rope - 1), jnp.bfloat16),
        ],
        axis=1,
    )
    bundle = jnp.concatenate(
        [
            key_values.reshape(-1, block, head_dim),
            jnp.moveaxis(latent.reshape(block, -1, BLOCK), 1, 0),
            tail[None],
        ],
        axis=0,
    )
    crossed = across_y(bundle, lax.axis_size("z") - REACH)
    k_part = lax.dynamic_slice_in_dim(key_up, group * GROUP, GROUP, 0).swapaxes(1, 2)
    v_part = lax.dynamic_slice_in_dim(value_up, group * GROUP, GROUP, 0)
    line = gather_z(jnp.stack([k_part, v_part]))

    last, one, two = two_behind(bundle, crossed)
    bundles = (two, one, bundle)
    line = after(line, last)
    at = jnp.stack([core.astype(jnp.int32), (place * block).astype(jnp.int32)])
    own = to_all(line, ("x", "y"))
    teach, bias = run_teacher(at, queries, bundles, latent.shape[1] // BLOCK)
    own = after(own, teach)
    other = partner(own)
    with_keys = (at, queries, query_pos.swapaxes(1, 2), bundles, bias, teach)
    earlier = run_student(*with_keys, own, 0)
    out, _, error = run_student(*with_keys, after(other, earlier[1]), 1, earlier)
    return out, error.reshape(block)


def solution(mesh):
    dp, ctx = mesh.devices.shape
    fine = Mesh(mesh.devices.reshape(dp // 2, 2, 4, ctx // 4), ("x", "core", "y", "z"))
    features = ("y", "z")
    tokens = ("x", "core", *features)
    placed = (
        P(None, tokens, None),
        P(None, tokens, None),
        P(None, None, tokens, None),
        P(tokens, None),
        P(tokens, None),
        P(None, None, features),
        P(None, features, None),
        P(tokens),
    )
    return jax.shard_map(
        shards,
        mesh=fine,
        in_specs=placed,
        out_specs=(P(None, tokens, None), P(tokens)),
        check_vma=False,
    )
```

```python
import functools
import math

import jax
import jax.numpy as jnp
from jax import lax
from jax.experimental import pallas as pl
from jax.experimental.pallas import tpu as pltpu
from jax.sharding import Mesh
from jax.sharding import PartitionSpec as P

REACH = 2
GROUP = 4
BLOCK = 128
MASKED = -1e30
CHAIN = 2
LOG2E = math.log2(math.e)


def to_all(a, axis):
    sizes = [lax.axis_size(k) for k in ((axis,) if isinstance(axis, str) else axis)]
    n = math.prod(sizes)
    got = lax.all_to_all(jnp.broadcast_to(a[None], (n, *a.shape)), axis, 0, 0, tiled=True)
    return got.reshape(*sizes, *a.shape)


def across_y(block, z_from):
    ny, nz = lax.axis_size("y"), lax.axis_size("z")
    route = [((y - 1) * nz + z, y * nz + z) for y in range(1, ny) for z in range(z_from, nz)]
    return lax.ppermute(block, ("y", "z"), route)


def two_behind(block, crossed):
    nz = lax.axis_size("z")
    z = lax.axis_index("z")
    last = jnp.where(z == nz - 1, crossed, block)
    one = lax.ppermute(last, "z", [(i, (i + 1) % nz) for i in range(nz)])
    two = lax.ppermute(one, "z", [(i, i + 1) for i in range(nz - 1)])
    wrapped = lax.ppermute(crossed, "z", [(nz - 2, 0)])
    return last, one, jnp.where(z == 0, wrapped, two)


def partner(a):
    return lax.ppermute(a, "core", [(0, 1), (1, 0)])


def gather_z(part):
    line = to_all(part, "z")
    line = jnp.transpose(line, (1, 2, 0, 3, 4))
    return line.reshape(*part.shape[:2], -1, part.shape[3])


def after(a, *others):
    return lax.optimization_barrier((a, *others))[0]


def nt(a, b):
    return lax.dot_general(a, b, (((1,), (1,)), ((), ())), preferred_element_type=jnp.float32)


def nn(a, b):
    return jnp.dot(a, b, preferred_element_type=jnp.float32)


def weights_of(scores, bias, scale):
    rows, keys = scores.shape
    t = (scores * (scale * LOG2E)).reshape(-1, BLOCK, keys) + bias[None]
    t = t.reshape(rows, keys)
    e = jnp.exp2(t - jnp.max(t, axis=-1, keepdims=True))
    return (e * (1.0 / jnp.sum(e, axis=-1, keepdims=True))).astype(jnp.bfloat16)


def teacher(rope, at_ref, q, kv2, kv1, kv0, la2, la1, la0, kp2, kp1, kp0, out, bias_out, lat_out, turned_out, bias):
    width = la0.shape[0] * BLOCK

    @pl.when(pl.program_id(0) == 0)
    def _():
        segs = []
        for b, (la, kp) in enumerate(((la2, kp2), (la1, kp1), (la0, kp0))):
            rows = slice(b * BLOCK, (b + 1) * BLOCK)
            for c in range(la.shape[0]):
                lat_out[rows, c * BLOCK : (c + 1) * BLOCK] = la[c]
                turned_out[c * BLOCK : (c + 1) * BLOCK, rows] = la[c].T
            both = kp[0]
            lane = lax.broadcasted_iota(jnp.int32, both.shape, 1)
            turned_out[width:, rows] = jnp.where(lane < rope, both, jnp.zeros_like(both)).T
            segs.append(jnp.broadcast_to(both[:, rope : rope + 1].astype(jnp.float32), (BLOCK, BLOCK)))
        window = len(segs) * BLOCK
        key_seg = jnp.concatenate([s.T for s in segs], axis=1)
        query_seg = jnp.concatenate([segs[-1]] * len(segs), axis=1)
        token = lax.broadcasted_iota(jnp.int32, (BLOCK, window), 0)
        key = lax.broadcasted_iota(jnp.int32, (BLOCK, window), 1) - REACH * BLOCK
        allowed = (key_seg == query_seg) & (key <= token) & (key + at_ref[1] >= 0)
        bias[...] = jnp.where(allowed, 0.0, MASKED)
        bias_out[...] = bias[...]

    head_dim = q.shape[-1]
    keys = jnp.concatenate([kv2[0], kv1[0], kv0[0]], axis=0)
    values = jnp.concatenate([kv2[1], kv1[1], kv0[1]], axis=0)
    p = weights_of(nt(q[...].reshape(GROUP * BLOCK, head_dim), keys), bias[...], head_dim**-0.5)
    out[...] = nn(p, values).astype(jnp.bfloat16).reshape(out.shape)


def run_teacher(at_ref, queries, bundles, chunks, rope):
    heads, block, head_dim = queries.shape
    kv_rows = bundles[0].shape[0] - chunks - 1
    per_kv = heads // (kv_rows // 2) // GROUP
    window = (REACH + 1) * BLOCK
    kv = pl.BlockSpec((2, BLOCK, BLOCK), lambda s, i: (s // per_kv, 0, 0))
    la = pl.BlockSpec((chunks, BLOCK, BLOCK), lambda s, i: (kv_rows // chunks, 0, 0))
    kp = pl.BlockSpec((1, BLOCK, BLOCK), lambda s, i: (kv_rows + chunks, 0, 0))
    group = pl.BlockSpec((GROUP, BLOCK, head_dim), lambda s, i: (s, 0, 0))
    once = [
        jax.ShapeDtypeStruct((BLOCK, window), jnp.float32),
        jax.ShapeDtypeStruct((window, chunks * BLOCK), jnp.bfloat16),
        jax.ShapeDtypeStruct(((chunks + 1) * BLOCK, window), jnp.bfloat16),
    ]
    return pl.pallas_call(
        functools.partial(teacher, rope),
        out_shape=[jax.ShapeDtypeStruct(queries.shape, jnp.bfloat16), *once],
        grid_spec=pltpu.PrefetchScalarGridSpec(
            num_scalar_prefetch=1,
            grid=(heads // GROUP,),
            in_specs=[group, kv, kv, kv, la, la, la, kp, kp, kp],
            out_specs=[group, *(pl.BlockSpec(o.shape, lambda s, i: (0, 0)) for o in once)],
            scratch_shapes=[pltpu.VMEM((BLOCK, window), jnp.float32)],
        ),
        cost_estimate=pl.CostEstimate(
            flops=4 * heads * block * window * head_dim, bytes_accessed=4 * 2**20, transcendentals=0
        ),
        name="teacher",
    )(at_ref, queries, *bundles, *bundles, *bundles)


def student(heads, at_ref, q, qpos, bias, lat, turned, teach, w, *refs):
    acc_in = refs[1] if len(refs) == 6 else None
    out, acc = refs[2:4] if acc_in is not None else refs[:2]
    ql = refs[-1]
    step = pl.program_id(0)
    width = lat.shape[1]
    count, _, _, rope, block = qpos.shape
    head_dim = q.shape[-1]

    @pl.when(step == 0)
    def _():
        acc[...] = jnp.zeros_like(acc) if acc_in is None else acc_in[...]
        ql[...] = jnp.zeros_like(ql)

    for k in range(count):
        for h in range(GROUP):
            rows = slice(h * block, (h + 1) * block)
            w_k = w[k, :, 0, h].reshape(width, head_dim)
            ql[k, rows, :width] = nt(q[k, 0, h], w_k).astype(jnp.bfloat16)
            ql[k, rows, width : width + rope] = qpos[k, 0, h].T
    scores = [nn(ql[k], turned[...]) for k in range(count)]
    total = acc[...]
    for k in range(count):
        p = weights_of(scores[k], bias[...], 1.0 / math.sqrt(head_dim + rope))
        low = nn(p, lat[...]).astype(jnp.bfloat16)
        for h in range(GROUP):
            w_v = w[k, :, 1, h].reshape(width, head_dim)
            o = nn(low[h * block : (h + 1) * block], w_v).astype(jnp.bfloat16)
            out[k, 0, h] = o
            d = o.astype(jnp.float32) - teach[k, 0, h].astype(jnp.float32)
            total = total + d * d
    acc[...] = total

    if acc_in is not None:

        @pl.when(step == pl.num_programs(0) - 1)
        def _():
            refs[4][...] = jnp.sum(acc[...].T, axis=0, keepdims=True) * (1.0 / (heads * head_dim))


def run_student(at_ref, queries, query_pos, bias, lat, turned, teach, w, other, earlier=()):
    heads, block, head_dim = queries.shape
    rope = query_pos.shape[1]
    nx = w.shape[0]
    grouped = (nx, 2, GROUP)
    whole = lambda a: pl.BlockSpec(a.shape, lambda s, at: (0,) * a.ndim)

    def of_group(rows, columns):
        place = lambda s, at: (s, 1 - at[0] if other else at[0], 0, 0, 0)
        return pl.BlockSpec((CHAIN, 1, GROUP, rows, columns), place)

    heads_spec = of_group(block, head_dim)
    sums = pl.BlockSpec((BLOCK, head_dim), lambda s, i: (0, 0))
    in_specs = [
        heads_spec,
        of_group(rope, block),
        whole(bias),
        whole(lat),
        whole(turned),
        heads_spec,
        pl.BlockSpec((CHAIN, *w.shape[1:]), lambda s, i: (s, 0, 0, 0, 0, 0)),
    ]
    shape = (*grouped, block, head_dim)
    out_shape = [
        jax.ShapeDtypeStruct(shape, jnp.bfloat16),
        jax.ShapeDtypeStruct((BLOCK, head_dim), jnp.float32),
    ]
    out_specs = [heads_spec, sums]
    aliases = {}
    if earlier:
        in_specs += [pl.BlockSpec(memory_space=pl.ANY), sums]
        out_shape.append(jax.ShapeDtypeStruct((1, BLOCK), jnp.float32))
        out_specs.append(pl.BlockSpec((1, BLOCK), lambda s, i: (0, 0)))
        aliases = {8: 0}
    flops = nx * GROUP * block * (4 * head_dim * lat.shape[1] + 2 * bias.shape[1] * (2 * lat.shape[1] + rope))
    return pl.pallas_call(
        functools.partial(student, heads),
        out_shape=out_shape,
        grid_spec=pltpu.PrefetchScalarGridSpec(
            num_scalar_prefetch=1,
            grid=(nx // CHAIN,),
            in_specs=in_specs,
            out_specs=out_specs,
            scratch_shapes=[pltpu.VMEM((CHAIN, GROUP * block, turned.shape[0]), jnp.bfloat16)],
        ),
        input_output_aliases=aliases,
        cost_estimate=pl.CostEstimate(flops=4 * flops, bytes_accessed=8 * 2**20, transcendentals=0),
        name="student",
    )(
        at_ref,
        queries.reshape(shape),
        query_pos.reshape(*grouped, rope, block),
        bias,
        lat,
        turned,
        teach.reshape(shape),
        w,
        *earlier,
    )


def shards(queries, query_pos, key_values, latent, key_pos, key_up, value_up, segment_ids):
    heads, block, head_dim = queries.shape
    rope = key_pos.shape[1]
    x, core = lax.axis_index("x"), lax.axis_index("core")
    place = lax.axis_index("y") * lax.axis_size("z") + lax.axis_index("z")
    group = x * 2 + core

    tail = jnp.concatenate(
        [
            key_pos,
            segment_ids.astype(jnp.bfloat16)[:, None],
            jnp.zeros((block, BLOCK - rope - 1), jnp.bfloat16),
        ],
        axis=1,
    )
    bundle = jnp.concatenate(
        [
            key_values.reshape(-1, block, head_dim),
            jnp.moveaxis(latent.reshape(block, -1, BLOCK), 1, 0),
            tail[None],
        ],
        axis=0,
    )
    crossed = across_y(bundle, lax.axis_size("z") - REACH)
    k_part = lax.dynamic_slice_in_dim(key_up, group * GROUP, GROUP, 0).swapaxes(1, 2)
    v_part = lax.dynamic_slice_in_dim(value_up, group * GROUP, GROUP, 0)
    line = gather_z(jnp.stack([k_part, v_part]))

    last, one, two = two_behind(bundle, crossed)
    bundles = (two, one, bundle)
    line = after(line, last)
    at = jnp.stack([core.astype(jnp.int32), (place * block).astype(jnp.int32)])
    own = to_all(line, ("x", "y"))
    teach, *fixed = run_teacher(at, queries, bundles, latent.shape[1] // BLOCK, rope)
    own = after(own, teach)
    other = partner(own)
    with_keys = (at, queries, query_pos.swapaxes(1, 2), *fixed, teach)
    earlier = run_student(*with_keys, own, 0)
    out, _, error = run_student(*with_keys, after(other, earlier[1]), 1, earlier)
    return out.reshape(queries.shape), error.reshape(block)


def solution(mesh):
    dp, ctx = mesh.devices.shape
    fine = Mesh(mesh.devices.reshape(dp // 2, 2, 4, ctx // 4), ("x", "core", "y", "z"))
    features = ("y", "z")
    tokens = ("x", "core", *features)
    placed = (
        P(None, tokens, None),
        P(None, tokens, None),
        P(None, None, tokens, None),
        P(tokens, None),
        P(tokens, None),
        P(None, None, features),
        P(None, features, None),
        P(tokens),
    )
    return jax.shard_map(
        shards,
        mesh=fine,
        in_specs=placed,
        out_specs=(P(None, tokens, None), P(tokens)),
        check_vma=False,
    )
```

```python
import functools
import math

import jax
import jax.numpy as jnp
from jax import lax
from jax.experimental import pallas as pl
from jax.experimental.pallas import tpu as pltpu
from jax.sharding import Mesh
from jax.sharding import PartitionSpec as P

REACH = 2
GROUP = 4
BLOCK = 128
MASKED = -1e30
LOG2E = math.log2(math.e)


def to_all(a, axis):
    sizes = [lax.axis_size(k) for k in ((axis,) if isinstance(axis, str) else axis)]
    n = math.prod(sizes)
    got = lax.all_to_all(jnp.broadcast_to(a[None], (n, *a.shape)), axis, 0, 0, tiled=True)
    return got.reshape(*sizes, *a.shape)


def across_y(block, z_from):
    ny, nz = lax.axis_size("y"), lax.axis_size("z")
    route = [((y - 1) * nz + z, y * nz + z) for y in range(1, ny) for z in range(z_from, nz)]
    return lax.ppermute(block, ("y", "z"), route)


def two_behind(block, crossed):
    nz = lax.axis_size("z")
    z = lax.axis_index("z")
    last = jnp.where(z == nz - 1, crossed, block)
    one = lax.ppermute(last, "z", [(i, (i + 1) % nz) for i in range(nz)])
    two = lax.ppermute(one, "z", [(i, i + 1) for i in range(nz - 1)])
    wrapped = lax.ppermute(crossed, "z", [(nz - 2, 0)])
    return last, one, jnp.where(z == 0, wrapped, two)


def partner(a):
    return lax.ppermute(a, "core", [(0, 1), (1, 0)])


def gather_z(part):
    line = to_all(part, "z")
    line = jnp.transpose(line, (1, 2, 0, 3, 4))
    return line.reshape(*part.shape[:2], -1, part.shape[3])


def after(a, *others):
    return lax.optimization_barrier((a, *others))[0]


def nt(a, b):
    return lax.dot_general(a, b, (((1,), (1,)), ((), ())), preferred_element_type=jnp.float32)


def nn(a, b):
    return jnp.dot(a, b, preferred_element_type=jnp.float32)


def weights_of(scores, bias, scale):
    rows, keys = scores.shape
    t = (scores * (scale * LOG2E)).reshape(-1, BLOCK, keys) + bias[None]
    t = t.reshape(rows, keys)
    e = jnp.exp2(t - jnp.max(t, axis=-1, keepdims=True))
    return (e * (1.0 / jnp.sum(e, axis=-1, keepdims=True))).astype(jnp.bfloat16)


def teacher(rope, at_ref, q, kv2, kv1, kv0, la2, la1, la0, kp2, kp1, kp0, out, bias_out, lat_out, turned_out, bias):
    width = la0.shape[0] * BLOCK

    @pl.when(pl.program_id(0) == 0)
    def _():
        segs = []
        for b, (la, kp) in enumerate(((la2, kp2), (la1, kp1), (la0, kp0))):
            rows = slice(b * BLOCK, (b + 1) * BLOCK)
            for c in range(la.shape[0]):
                lat_out[rows, c * BLOCK : (c + 1) * BLOCK] = la[c]
                turned_out[c * BLOCK : (c + 1) * BLOCK, rows] = la[c].T
            both = kp[0]
            lane = lax.broadcasted_iota(jnp.int32, both.shape, 1)
            turned_out[width:, rows] = jnp.where(lane < rope, both, jnp.zeros_like(both)).T
            segs.append(jnp.broadcast_to(both[:, rope : rope + 1].astype(jnp.float32), (BLOCK, BLOCK)))
        window = len(segs) * BLOCK
        key_seg = jnp.concatenate([s.T for s in segs], axis=1)
        query_seg = jnp.concatenate([segs[-1]] * len(segs), axis=1)
        token = lax.broadcasted_iota(jnp.int32, (BLOCK, window), 0)
        key = lax.broadcasted_iota(jnp.int32, (BLOCK, window), 1) - REACH * BLOCK
        allowed = (key_seg == query_seg) & (key <= token) & (key + at_ref[1] >= 0)
        bias[...] = jnp.where(allowed, 0.0, MASKED)
        bias_out[...] = bias[...]

    head_dim = q.shape[-1]
    keys = jnp.concatenate([kv2[0], kv1[0], kv0[0]], axis=0)
    values = jnp.concatenate([kv2[1], kv1[1], kv0[1]], axis=0)
    p = weights_of(nt(q[...].reshape(GROUP * BLOCK, head_dim), keys), bias[...], head_dim**-0.5)
    out[...] = nn(p, values).astype(jnp.bfloat16).reshape(out.shape)


def run_teacher(at_ref, queries, bundles, chunks, rope):
    heads, block, head_dim = queries.shape
    kv_rows = bundles[0].shape[0] - chunks - 1
    per_kv = heads // (kv_rows // 2) // GROUP
    window = (REACH + 1) * BLOCK
    kv = pl.BlockSpec((2, BLOCK, BLOCK), lambda s, i: (s // per_kv, 0, 0))
    la = pl.BlockSpec((chunks, BLOCK, BLOCK), lambda s, i: (kv_rows // chunks, 0, 0))
    kp = pl.BlockSpec((1, BLOCK, BLOCK), lambda s, i: (kv_rows + chunks, 0, 0))
    group = pl.BlockSpec((GROUP, BLOCK, head_dim), lambda s, i: (s, 0, 0))
    once = [
        jax.ShapeDtypeStruct((BLOCK, window), jnp.float32),
        jax.ShapeDtypeStruct((window, chunks * BLOCK), jnp.bfloat16),
        jax.ShapeDtypeStruct(((chunks + 1) * BLOCK, window), jnp.bfloat16),
    ]
    return pl.pallas_call(
        functools.partial(teacher, rope),
        out_shape=[jax.ShapeDtypeStruct(queries.shape, jnp.bfloat16), *once],
        grid_spec=pltpu.PrefetchScalarGridSpec(
            num_scalar_prefetch=1,
            grid=(heads // GROUP,),
            in_specs=[group, kv, kv, kv, la, la, la, kp, kp, kp],
            out_specs=[group, *(pl.BlockSpec(o.shape, lambda s, i: (0, 0)) for o in once)],
            scratch_shapes=[pltpu.VMEM((BLOCK, window), jnp.float32)],
        ),
        cost_estimate=pl.CostEstimate(
            flops=4 * heads * block * window * head_dim, bytes_accessed=4 * 2**20, transcendentals=0
        ),
        name="teacher",
    )(at_ref, queries, *bundles, *bundles, *bundles)


def student(heads, sources, ends, at_ref, q, qpos, bias, lat, turned, teach, *refs):
    count = sum(sources)
    held, refs = refs[:count], refs[count:]
    first, last = ends
    acc_in = None if first else refs[1]
    refs = refs if first else refs[2:]
    out, acc = refs[:2]
    ql, low = refs[-2:]
    step = pl.program_id(0)
    width = lat.shape[1]
    rope, block = qpos.shape[-2:]
    head_dim = q.shape[-1]

    @pl.when(step == 0)
    def _():
        acc[...] = jnp.zeros_like(acc) if first else acc_in[...]
        ql[...] = jnp.zeros_like(ql)

    def at_step(do):
        at = 0
        for k, parts in enumerate(sources):
            mine = held[at : at + parts]
            at += parts
            if len(sources) == 1:
                do(mine)
            else:
                pl.when(step == k)(functools.partial(do, mine))

    def lift(mine):
        for h in range(GROUP):
            rows = slice(h * block, (h + 1) * block)
            col = 0
            for w in mine:
                n = w.shape[0] * block
                ql[rows, col : col + n] = nt(q[0, 0, h], w[:, 0, h].reshape(n, head_dim)).astype(jnp.bfloat16)
                col += n
            ql[rows, width : width + rope] = qpos[0, 0, h].T

    def drop(mine):
        total = acc[...]
        for h in range(GROUP):
            w = jnp.concatenate([r[:, 1, h].reshape(r.shape[0] * block, head_dim) for r in mine], axis=0)
            o = nn(low[h * block : (h + 1) * block], w).astype(jnp.bfloat16)
            out[0, 0, h] = o
            d = o.astype(jnp.float32) - teach[0, 0, h].astype(jnp.float32)
            total = total + d * d
        acc[...] = total

    at_step(lift)
    p = weights_of(nn(ql[...], turned[...]), bias[...], 1.0 / math.sqrt(head_dim + rope))
    low[...] = nn(p, lat[...]).astype(jnp.bfloat16)
    at_step(drop)

    if last:

        @pl.when(step == pl.num_programs(0) - 1)
        def _():
            refs[2][...] = jnp.sum(acc[...].T, axis=0, keepdims=True) * (1.0 / (heads * head_dim))


def run_student(at_ref, queries, query_pos, bias, lat, turned, teach, held, places, other, earlier=(), last=False):
    heads, block, head_dim = queries.shape
    rope = query_pos.shape[1]
    nx = heads // GROUP // 2
    grouped = (nx, 2, GROUP)
    flat = [w for parts in held for w in parts]

    def whole(a):
        return pl.BlockSpec(a.shape, lambda s, at: (0,) * a.ndim)

    def position(s, at):
        place = places[0]
        for k in range(1, len(places)):
            place = jnp.where(s == k, places[k], place)
        return ((at[2] + place) % nx, 1 - at[0] if other else at[0], 0, 0, 0)

    def of_group(rows, columns):
        return pl.BlockSpec((1, 1, GROUP, rows, columns), position)

    heads_spec = of_group(block, head_dim)
    sums = pl.BlockSpec((BLOCK, head_dim), lambda s, i: (0, 0))
    in_specs = [heads_spec, of_group(rope, block), whole(bias), whole(lat), whole(turned), heads_spec]
    in_specs += [whole(w) for w in flat]
    shape = (*grouped, block, head_dim)
    out_shape = [
        jax.ShapeDtypeStruct(shape, jnp.bfloat16),
        jax.ShapeDtypeStruct((BLOCK, head_dim), jnp.float32),
    ]
    out_specs = [heads_spec, sums]
    aliases = {}
    if earlier:
        aliases = {1 + len(in_specs): 0}
        in_specs += [pl.BlockSpec(memory_space=pl.ANY), sums]
    if last:
        out_shape.append(jax.ShapeDtypeStruct((1, BLOCK), jnp.float32))
        out_specs.append(pl.BlockSpec((1, BLOCK), lambda s, i: (0, 0)))
    rows = GROUP * block
    flops = len(held) * rows * (4 * head_dim * lat.shape[1] + 2 * bias.shape[1] * (2 * lat.shape[1] + rope))
    return pl.pallas_call(
        functools.partial(student, heads, tuple(len(h) for h in held), (not earlier, last)),
        out_shape=out_shape,
        grid_spec=pltpu.PrefetchScalarGridSpec(
            num_scalar_prefetch=1,
            grid=(len(held),),
            in_specs=in_specs,
            out_specs=out_specs,
            scratch_shapes=[
                pltpu.VMEM((rows, turned.shape[0]), jnp.bfloat16),
                pltpu.VMEM((rows, lat.shape[1]), jnp.bfloat16),
            ],
        ),
        input_output_aliases=aliases,
        cost_estimate=pl.CostEstimate(flops=4 * flops, bytes_accessed=8 * 2**20, transcendentals=0),
        name="student",
    )(
        at_ref,
        queries.reshape(shape),
        query_pos.reshape(*grouped, rope, block),
        bias,
        lat,
        turned,
        teach.reshape(shape),
        *flat,
        *earlier[:2],
    )


def along_x(a, by):
    n = lax.axis_size("x")
    return lax.ppermute(a, "x", [((i + by) % n, i) for i in range(n)])


def shards(queries, query_pos, key_values, latent, key_pos, key_up, value_up, segment_ids):
    heads, block, head_dim = queries.shape
    rope = key_pos.shape[1]
    x, core = lax.axis_index("x"), lax.axis_index("core")
    place = lax.axis_index("y") * lax.axis_size("z") + lax.axis_index("z")
    group = x * 2 + core

    tail = jnp.concatenate(
        [
            key_pos,
            segment_ids.astype(jnp.bfloat16)[:, None],
            jnp.zeros((block, BLOCK - rope - 1), jnp.bfloat16),
        ],
        axis=1,
    )
    bundle = jnp.concatenate(
        [
            key_values.reshape(-1, block, head_dim),
            jnp.moveaxis(latent.reshape(block, -1, BLOCK), 1, 0),
            tail[None],
        ],
        axis=0,
    )
    crossed = across_y(bundle, lax.axis_size("z") - REACH)
    k_part = lax.dynamic_slice_in_dim(key_up, group * GROUP, GROUP, 0).swapaxes(1, 2)
    v_part = lax.dynamic_slice_in_dim(value_up, group * GROUP, GROUP, 0)
    line = gather_z(jnp.stack([k_part, v_part]))

    last, one, two = two_behind(bundle, crossed)
    bundles = (two, one, bundle)
    at = jnp.stack([core.astype(jnp.int32), (place * block).astype(jnp.int32), x.astype(jnp.int32)])
    own = after(to_all(after(line, last), "y"), one)
    half = own.shape[0] // 2
    plus, minus = along_x(own, 1), along_x(own, -1)
    teach, *fixed = run_teacher(at, queries, bundles, latent.shape[1] // BLOCK, rope)
    plus, minus = after(plus, teach), after(minus, teach)
    cut = (plus[:half], minus[half:])
    far = (along_x(cut[0], 1), along_x(cut[1], -1))
    near = [(own,), (plus,), (minus,)]
    near_2 = [(partner(own),), (partner(after(plus, *cut)),), (partner(after(minus, *cut)),)]

    with_keys = (at, queries, query_pos.swapaxes(1, 2), *fixed, teach)
    done = run_student(*with_keys, near, (0, 1, 3), 0)
    done = run_student(*with_keys, near_2, (0, 1, 3), 1, done)
    far = tuple(after(w, done[1]) for w in far)
    far_2 = tuple(partner(w) for w in far)
    done = run_student(*with_keys, [far], (2,), 0, done)
    out, _, error = run_student(*with_keys, [far_2], (2,), 1, done, True)
    return out.reshape(queries.shape), error.reshape(block)


def solution(mesh):
    dp, ctx = mesh.devices.shape
    fine = Mesh(mesh.devices.reshape(dp // 2, 2, 4, ctx // 4), ("x", "core", "y", "z"))
    features = ("y", "z")
    tokens = ("x", "core", *features)
    placed = (
        P(None, tokens, None),
        P(None, tokens, None),
        P(None, None, tokens, None),
        P(tokens, None),
        P(tokens, None),
        P(None, None, features),
        P(None, features, None),
        P(tokens),
    )
    return jax.shard_map(
        shards,
        mesh=fine,
        in_specs=placed,
        out_specs=(P(None, tokens, None), P(tokens)),
        check_vma=False,
    )
```

```python
import functools
import math

import jax
import jax.numpy as jnp
from jax import lax
from jax.experimental import pallas as pl
from jax.experimental.pallas import tpu as pltpu
from jax.sharding import Mesh
from jax.sharding import PartitionSpec as P

REACH = 2
GROUP = 4
BLOCK = 128
MASKED = -1e30
CHAIN = 2
LOG2E = math.log2(math.e)


def to_all(a, axis):
    sizes = [lax.axis_size(k) for k in ((axis,) if isinstance(axis, str) else axis)]
    n = math.prod(sizes)
    got = lax.all_to_all(jnp.broadcast_to(a[None], (n, *a.shape)), axis, 0, 0, tiled=True)
    return got.reshape(*sizes, *a.shape)


def across_y(block, z_from):
    ny, nz = lax.axis_size("y"), lax.axis_size("z")
    route = [((y - 1) * nz + z, y * nz + z) for y in range(1, ny) for z in range(z_from, nz)]
    return lax.ppermute(block, ("y", "z"), route)


def two_behind(block, crossed):
    nz = lax.axis_size("z")
    z = lax.axis_index("z")
    last = jnp.where(z == nz - 1, crossed, block)
    one = lax.ppermute(last, "z", [(i, (i + 1) % nz) for i in range(nz)])
    two = lax.ppermute(one, "z", [(i, i + 1) for i in range(nz - 1)])
    wrapped = lax.ppermute(crossed, "z", [(nz - 2, 0)])
    return last, one, jnp.where(z == 0, wrapped, two)


def partner(a):
    return lax.ppermute(a, "core", [(0, 1), (1, 0)])


def gather_z(part):
    line = to_all(part, "z")
    line = jnp.transpose(line, (1, 2, 0, 3, 4))
    return line.reshape(*part.shape[:2], -1, part.shape[3])


def after(a, *others):
    return lax.optimization_barrier((a, *others))[0]


def nt(a, b):
    return lax.dot_general(a, b, (((1,), (1,)), ((), ())), preferred_element_type=jnp.float32)


def nn(a, b):
    return jnp.dot(a, b, preferred_element_type=jnp.float32)


def weights_of(scores, bias, scale):
    rows, keys = scores.shape
    t = (scores * (scale * LOG2E)).reshape(-1, BLOCK, keys) + bias[None]
    t = t.reshape(rows, keys)
    e = jnp.exp2(t - jnp.max(t, axis=-1, keepdims=True))
    return (e * (1.0 / jnp.sum(e, axis=-1, keepdims=True))).astype(jnp.bfloat16)


def teacher(rope, at_ref, q, kv2, kv1, kv0, la2, la1, la0, kp2, kp1, kp0, out, bias_out, lat_out, turned_out, bias):
    width = la0.shape[0] * BLOCK

    @pl.when(pl.program_id(0) == 0)
    def _():
        segs = []
        for b, (la, kp) in enumerate(((la2, kp2), (la1, kp1), (la0, kp0))):
            rows = slice(b * BLOCK, (b + 1) * BLOCK)
            for c in range(la.shape[0]):
                lat_out[rows, c * BLOCK : (c + 1) * BLOCK] = la[c]
                turned_out[c * BLOCK : (c + 1) * BLOCK, rows] = la[c].T
            both = kp[0]
            lane = lax.broadcasted_iota(jnp.int32, both.shape, 1)
            turned_out[width:, rows] = jnp.where(lane < rope, both, jnp.zeros_like(both)).T
            segs.append(jnp.broadcast_to(both[:, rope : rope + 1].astype(jnp.float32), (BLOCK, BLOCK)))
        window = len(segs) * BLOCK
        key_seg = jnp.concatenate([s.T for s in segs], axis=1)
        query_seg = jnp.concatenate([segs[-1]] * len(segs), axis=1)
        token = lax.broadcasted_iota(jnp.int32, (BLOCK, window), 0)
        key = lax.broadcasted_iota(jnp.int32, (BLOCK, window), 1) - REACH * BLOCK
        allowed = (key_seg == query_seg) & (key <= token) & (key + at_ref[1] >= 0)
        bias[...] = jnp.where(allowed, 0.0, MASKED)
        bias_out[...] = bias[...]

    head_dim = q.shape[-1]
    keys = jnp.concatenate([kv2[0], kv1[0], kv0[0]], axis=0)
    values = jnp.concatenate([kv2[1], kv1[1], kv0[1]], axis=0)
    p = weights_of(nt(q[...].reshape(GROUP * BLOCK, head_dim), keys), bias[...], head_dim**-0.5)
    out[...] = nn(p, values).astype(jnp.bfloat16).reshape(out.shape)


def run_teacher(at_ref, queries, bundles, chunks, rope):
    heads, block, head_dim = queries.shape
    kv_rows = bundles[0].shape[0] - chunks - 1
    per_kv = heads // (kv_rows // 2) // GROUP
    window = (REACH + 1) * BLOCK
    kv = pl.BlockSpec((2, BLOCK, BLOCK), lambda s, i: (s // per_kv, 0, 0))
    la = pl.BlockSpec((chunks, BLOCK, BLOCK), lambda s, i: (kv_rows // chunks, 0, 0))
    kp = pl.BlockSpec((1, BLOCK, BLOCK), lambda s, i: (kv_rows + chunks, 0, 0))
    group = pl.BlockSpec((GROUP, BLOCK, head_dim), lambda s, i: (s, 0, 0))
    once = [
        jax.ShapeDtypeStruct((BLOCK, window), jnp.float32),
        jax.ShapeDtypeStruct((window, chunks * BLOCK), jnp.bfloat16),
        jax.ShapeDtypeStruct(((chunks + 1) * BLOCK, window), jnp.bfloat16),
    ]
    return pl.pallas_call(
        functools.partial(teacher, rope),
        out_shape=[jax.ShapeDtypeStruct(queries.shape, jnp.bfloat16), *once],
        grid_spec=pltpu.PrefetchScalarGridSpec(
            num_scalar_prefetch=1,
            grid=(heads // GROUP,),
            in_specs=[group, kv, kv, kv, la, la, la, kp, kp, kp],
            out_specs=[group, *(pl.BlockSpec(o.shape, lambda s, i: (0, 0)) for o in once)],
            scratch_shapes=[pltpu.VMEM((BLOCK, window), jnp.float32)],
        ),
        cost_estimate=pl.CostEstimate(
            flops=4 * heads * block * window * head_dim, bytes_accessed=4 * 2**20, transcendentals=0
        ),
        name="teacher",
    )(at_ref, queries, *bundles, *bundles, *bundles)


def student(heads, at_ref, q, qpos, bias, lat, turned, teach, w, *refs):
    acc_in = refs[1] if len(refs) == 6 else None
    out, acc = refs[2:4] if acc_in is not None else refs[:2]
    ql = refs[-1]
    step = pl.program_id(0)
    width = lat.shape[1]
    count, _, _, rope, block = qpos.shape
    head_dim = q.shape[-1]

    @pl.when(step == 0)
    def _():
        acc[...] = jnp.zeros_like(acc) if acc_in is None else acc_in[...]
        ql[...] = jnp.zeros_like(ql)

    for k in range(count):
        for h in range(GROUP):
            rows = slice(h * block, (h + 1) * block)
            w_k = w[:, k, 0, h].reshape(width, head_dim)
            ql[k, rows, :width] = nt(w_k, q[k, 0, h]).T.astype(jnp.bfloat16)
            ql[k, rows, width : width + rope] = qpos[k, 0, h].T
    scores = [nn(ql[k], turned[...]) for k in range(count)]
    total = acc[...]
    for k in range(count):
        p = weights_of(scores[k], bias[...], 1.0 / math.sqrt(head_dim + rope))
        low = nn(p, lat[...]).astype(jnp.bfloat16)
        for h in range(GROUP):
            w_v = w[:, k, 1, h].reshape(width, head_dim)
            o = nn(low[h * block : (h + 1) * block], w_v).astype(jnp.bfloat16)
            out[k, 0, h] = o
            d = o.astype(jnp.float32) - teach[k, 0, h].astype(jnp.float32)
            total = total + d * d
    acc[...] = total

    if acc_in is not None:

        @pl.when(step == pl.num_programs(0) - 1)
        def _():
            refs[4][...] = jnp.sum(acc[...].T, axis=0, keepdims=True) * (1.0 / (heads * head_dim))


def run_student(at_ref, queries, query_pos, bias, lat, turned, teach, w, other, earlier=()):
    heads, block, head_dim = queries.shape
    rope = query_pos.shape[1]
    nx = w.shape[1]
    grouped = (nx, 2, GROUP)
    whole = lambda a: pl.BlockSpec(a.shape, lambda s, at: (0,) * a.ndim)

    def of_group(rows, columns):
        place = lambda s, at: (s, 1 - at[0] if other else at[0], 0, 0, 0)
        return pl.BlockSpec((CHAIN, 1, GROUP, rows, columns), place)

    heads_spec = of_group(block, head_dim)
    sums = pl.BlockSpec((BLOCK, head_dim), lambda s, i: (0, 0))
    in_specs = [
        heads_spec,
        of_group(rope, block),
        whole(bias),
        whole(lat),
        whole(turned),
        heads_spec,
        pl.BlockSpec((w.shape[0], CHAIN, *w.shape[2:]), lambda s, i: (0, s, 0, 0, 0, 0)),
    ]
    shape = (*grouped, block, head_dim)
    out_shape = [
        jax.ShapeDtypeStruct(shape, jnp.bfloat16),
        jax.ShapeDtypeStruct((BLOCK, head_dim), jnp.float32),
    ]
    out_specs = [heads_spec, sums]
    aliases = {}
    if earlier:
        in_specs += [pl.BlockSpec(memory_space=pl.ANY), sums]
        out_shape.append(jax.ShapeDtypeStruct((1, BLOCK), jnp.float32))
        out_specs.append(pl.BlockSpec((1, BLOCK), lambda s, i: (0, 0)))
        aliases = {8: 0}
    flops = nx * GROUP * block * (4 * head_dim * lat.shape[1] + 2 * bias.shape[1] * (2 * lat.shape[1] + rope))
    return pl.pallas_call(
        functools.partial(student, heads),
        out_shape=out_shape,
        grid_spec=pltpu.PrefetchScalarGridSpec(
            num_scalar_prefetch=1,
            grid=(nx // CHAIN,),
            in_specs=in_specs,
            out_specs=out_specs,
            scratch_shapes=[pltpu.VMEM((CHAIN, GROUP * block, turned.shape[0]), jnp.bfloat16)],
        ),
        input_output_aliases=aliases,
        cost_estimate=pl.CostEstimate(flops=4 * flops, bytes_accessed=8 * 2**20, transcendentals=0),
        name="student",
    )(
        at_ref,
        queries.reshape(shape),
        query_pos.reshape(*grouped, rope, block),
        bias,
        lat,
        turned,
        teach.reshape(shape),
        w,
        *earlier,
    )


def shards(queries, query_pos, key_values, latent, key_pos, key_up, value_up, segment_ids):
    heads, block, head_dim = queries.shape
    rope = key_pos.shape[1]
    x, core = lax.axis_index("x"), lax.axis_index("core")
    place = lax.axis_index("y") * lax.axis_size("z") + lax.axis_index("z")
    group = x * 2 + core

    tail = jnp.concatenate(
        [
            key_pos,
            segment_ids.astype(jnp.bfloat16)[:, None],
            jnp.zeros((block, BLOCK - rope - 1), jnp.bfloat16),
        ],
        axis=1,
    )
    bundle = jnp.concatenate(
        [
            key_values.reshape(-1, block, head_dim),
            jnp.moveaxis(latent.reshape(block, -1, BLOCK), 1, 0),
            tail[None],
        ],
        axis=0,
    )
    crossed = across_y(bundle, lax.axis_size("z") - REACH)
    k_part = lax.dynamic_slice_in_dim(key_up, group * GROUP, GROUP, 0).swapaxes(1, 2)
    v_part = lax.dynamic_slice_in_dim(value_up, group * GROUP, GROUP, 0)
    line = gather_z(jnp.stack([k_part, v_part]))

    last, one, two = two_behind(bundle, crossed)
    bundles = (two, one, bundle)
    line = after(line, last)
    at = jnp.stack([core.astype(jnp.int32), (place * block).astype(jnp.int32)])
    own = to_all(line, ("y", "x"))
    teach, *fixed = run_teacher(at, queries, bundles, latent.shape[1] // BLOCK, rope)
    own = after(own, teach)
    other = partner(own)
    with_keys = (at, queries, query_pos.swapaxes(1, 2), *fixed, teach)
    earlier = run_student(*with_keys, own, 0)
    out, _, error = run_student(*with_keys, after(other, earlier[1]), 1, earlier)
    return out.reshape(queries.shape), error.reshape(block)


def solution(mesh):
    dp, ctx = mesh.devices.shape
    fine = Mesh(mesh.devices.reshape(dp // 2, 2, 4, ctx // 4), ("x", "core", "y", "z"))
    features = ("y", "z")
    tokens = ("x", "core", *features)
    placed = (
        P(None, tokens, None),
        P(None, tokens, None),
        P(None, None, tokens, None),
        P(tokens, None),
        P(tokens, None),
        P(None, None, features),
        P(None, features, None),
        P(tokens),
    )
    return jax.shard_map(
        shards,
        mesh=fine,
        in_specs=placed,
        out_specs=(P(None, tokens, None), P(tokens)),
        check_vma=False,
    )
```
